32 devices in a mesh: dp: 2 (over x), pool: 4 (over z), ep: 4 (over y, core).
Axes of the slice: x: 2, y: 2, z: 4, core: 2. Of those that a mesh axis runs over, the one named last changes fastest.
Arguments:
- hidden: bfloat16 [4096, 896], P(('dp', 'pool', 'ep')), parts along dimension 0
- k_cache: bfloat16 [2, 4096, 32, 4, 128], P(None, ('dp', 'pool', 'ep')), parts along dimension 1
- v_cache: bfloat16 [2, 4096, 32, 4, 128], P(None, ('dp', 'pool', 'ep')), parts along dimension 1
- lengths: int32 [4096], P(('dp', 'pool', 'ep')), parts along dimension 0
- w_query: bfloat16 [2, 896, 2048], replicated
- w_key: bfloat16 [2, 896, 512], replicated
- w_value: bfloat16 [2, 896, 512], replicated
- w_out: bfloat16 [2, 2048, 896], replicated
- w_router: float32 [2, 896, 256], replicated
- expert_ids: int32 [2, 4096, 8], P(None, ('dp', 'pool', 'ep')), parts along dimension 1
- w_gate: bfloat16 [2, 256, 896, 256], P(None, ('pool', 'ep'))
- w_up: bfloat16 [2, 256, 896, 256], P(None, ('pool', 'ep'))
- w_down: bfloat16 [2, 256, 256, 896], P(None, ('pool', 'ep'))
Outputs:
- output: bfloat16 [4096, 896], P(('dp', 'pool', 'ep')), parts along dimension 0
There are 2 independent parts. The reference program is written for one: setup_inputs(seed, part) draws one part's arguments, and reference() takes and returns one part's arrays. A program takes and returns all parts, laid end to end along the dimension named above; an argument that names none is the same for every part.
All inputs are finite; a program needn't handle non-finite values.
Results may differ from the reference program's by a relative error of at most 0.02.
Values are sent between devices in bfloat16 or wider.
A program may use at most 1 GiB of HBM per device.

```python
import jax
import jax.numpy as jnp
from jax import lax

D = 896
HEADS = 16
KV_HEADS = 4
HEAD = 128
EXPERTS = 256
TOP = 8
FF = 256
TOK_DEV = 128
SEQ_LEN = 32
GROUP = 16
LAYERS = 2
ATT_BLOCK = 8

TOKENS = GROUP * TOK_DEV
LOCAL_EXPERTS = EXPERTS // GROUP
PAIR_MEAN = TOK_DEV * TOP // GROUP
LINK_CAP = 2 * PAIR_MEAN - 1
EXPERT_CAP = GROUP * ((LINK_CAP + LOCAL_EXPERTS - 1) // LOCAL_EXPERTS)
PER_KV = HEADS // KV_HEADS
EPS = 1e-6
ATTN_SCALE = HEAD ** -0.5


def source_routing(counts, rng_key):
    flat_ids = jnp.repeat(jnp.arange(EXPERTS, dtype=jnp.int32), counts, total_repeat_length=TOK_DEV * TOP)
    laid_out = flat_ids.reshape(TOP, TOK_DEV).T
    return laid_out[jax.random.permutation(rng_key, TOK_DEV)]


def layer_routing(rng_key):
    order_key, spread_key, offset_key, token_key = jax.random.split(rng_key, 4)
    half_group = GROUP // 2
    device_order = jax.random.permutation(order_key, GROUP)
    hot_dev = device_order[:half_group]
    cold_dev = device_order[half_group:]
    spread = jax.random.randint(spread_key, (GROUP, half_group), 0, PAIR_MEAN)
    spread = spread.at[:, 0].set(PAIR_MEAN - 1)
    link_count = jnp.zeros((GROUP, GROUP), jnp.int32)
    link_count = link_count.at[:, hot_dev].set(PAIR_MEAN + spread)
    link_count = link_count.at[:, cold_dev].set(PAIR_MEAN - spread)
    offsets = jax.random.randint(offset_key, (GROUP, GROUP), 0, LOCAL_EXPERTS)
    offsets = offsets.at[:, hot_dev[0]].set(0)
    local_idx = jnp.arange(LOCAL_EXPERTS)
    extra_one = ((local_idx[None, None, :] - offsets[:, :, None]) % LOCAL_EXPERTS) < (link_count % LOCAL_EXPERTS)[:, :, None]
    expert_count = (link_count // LOCAL_EXPERTS)[:, :, None] + extra_one.astype(jnp.int32)
    token_keys = jax.random.split(token_key, GROUP)
    routed = jax.vmap(source_routing)(expert_count.reshape(GROUP, EXPERTS), token_keys)
    return routed.reshape(TOKENS, TOP)


def draw_lengths(rng_key):
    lengths = jax.random.randint(rng_key, (TOKENS,), SEQ_LEN // 2, SEQ_LEN + 1)
    return lengths.at[0].set(SEQ_LEN).at[1].set(SEQ_LEN // 2)


def setup_inputs(seed: int = 0, part: int = 0) -> dict:
    base_key = jax.random.key(seed)
    shared_keys = jax.random.split(base_key, 8)
    part_keys = jax.random.split(jax.random.fold_in(base_key, part), 5)
    cache_shape = (LAYERS, TOKENS, SEQ_LEN, KV_HEADS, HEAD)
    hidden = jax.random.normal(part_keys[0], (TOKENS, D), jnp.float32).astype(jnp.bfloat16)
    k_cache = jax.random.normal(part_keys[1], cache_shape, jnp.float32).astype(jnp.bfloat16)
    v_cache = jax.random.normal(part_keys[2], cache_shape, jnp.float32).astype(jnp.bfloat16)
    lengths = draw_lengths(part_keys[3])
    expert_ids = jax.vmap(layer_routing)(jax.random.split(part_keys[4], LAYERS))
    w_query = (jax.random.normal(shared_keys[0], (LAYERS, D, HEADS * HEAD), jnp.float32) * D ** -0.5).astype(jnp.bfloat16)
    w_key = (jax.random.normal(shared_keys[1], (LAYERS, D, KV_HEADS * HEAD), jnp.float32) * D ** -0.5).astype(jnp.bfloat16)
    w_value = (jax.random.normal(shared_keys[2], (LAYERS, D, KV_HEADS * HEAD), jnp.float32) * D ** -0.5).astype(jnp.bfloat16)
    w_out = (jax.random.normal(shared_keys[3], (LAYERS, HEADS * HEAD, D), jnp.float32) * (0.4 * (SEQ_LEN / (HEADS * HEAD)) ** 0.5)).astype(jnp.bfloat16)
    w_router = jax.random.normal(shared_keys[4], (LAYERS, D, EXPERTS), jnp.float32) * (1.5 * D ** -0.5)
    w_gate = (jax.random.normal(shared_keys[5], (LAYERS, EXPERTS, D, FF), jnp.float32) * D ** -0.5).astype(jnp.bfloat16)
    w_up = (jax.random.normal(shared_keys[6], (LAYERS, EXPERTS, D, FF), jnp.float32) * D ** -0.5).astype(jnp.bfloat16)
    w_down = (jax.random.normal(shared_keys[7], (LAYERS, EXPERTS, FF, D), jnp.float32) * (TOP / FF) ** 0.5).astype(jnp.bfloat16)
    return {"hidden": hidden, "k_cache": k_cache, "v_cache": v_cache, "lengths": lengths, "w_query": w_query, "w_key": w_key, "w_value": w_value, "w_out": w_out, "w_router": w_router, "expert_ids": expert_ids, "w_gate": w_gate, "w_up": w_up, "w_down": w_down}


def rms_norm(values):
    wide = values.astype(jnp.float32)
    inv_norm = lax.rsqrt(jnp.mean(wide * wide, axis=-1, keepdims=True) + EPS)
    return (wide * inv_norm).astype(jnp.bfloat16)


def attend_block(block):
    query, keys_blk, values_blk, len_blk, key_new, value_new = block
    query = query.astype(jnp.float32)
    scores = jnp.einsum('tkgd,tskd->tkgs', query, keys_blk.astype(jnp.float32)) * ATTN_SCALE
    valid_pos = jnp.arange(SEQ_LEN)[None, :] < len_blk[:, None]
    scores = jnp.where(valid_pos[:, None, None, :], scores, -jnp.inf)
    score_new = jnp.einsum('tkgd,tkd->tkg', query, key_new.astype(jnp.float32)) * ATTN_SCALE
    peak_score = jnp.maximum(jnp.max(scores, axis=-1), score_new)
    att_probs = jnp.exp(scores - peak_score[..., None])
    new_prob = jnp.exp(score_new - peak_score)
    norm_total = jnp.sum(att_probs, axis=-1) + new_prob
    att_probs = (att_probs / norm_total[..., None]).astype(jnp.bfloat16)
    new_prob = (new_prob / norm_total).astype(jnp.bfloat16)
    mixed = jnp.einsum('tkgs,tskd->tkgd', att_probs.astype(jnp.float32), values_blk.astype(jnp.float32))
    mixed = mixed + new_prob.astype(jnp.float32)[..., None] * value_new.astype(jnp.float32)[:, :, None, :]
    return mixed.astype(jnp.bfloat16)


def expert_mix(routed, layer_ids, gates, g_weight, u_weight, d_weight):
    flat_ids = layer_ids.reshape(-1)
    pair_count = TOKENS * TOP
    sort_order = jnp.argsort(flat_ids, stable=True)
    sorted_ids = flat_ids[sort_order]
    counts = jnp.bincount(flat_ids, length=EXPERTS)
    starts = jnp.cumsum(counts) - counts
    ranks = jnp.arange(pair_count) - starts[sorted_ids]
    pair_for_slot = jnp.full((EXPERTS * EXPERT_CAP,), pair_count, jnp.int32)
    pair_for_slot = pair_for_slot.at[sorted_ids * EXPERT_CAP + ranks].set(sort_order.astype(jnp.int32), mode='drop')
    flat_gates = gates.reshape(-1)

    def expert_body(carry, item):
        gate_w, up_w, down_w, pair_idx = item
        token_idx = pair_idx // TOP
        rows = jnp.take(routed, token_idx, axis=0, mode='fill', fill_value=0)
        first = jnp.dot(rows, gate_w, preferred_element_type=jnp.float32)
        second = jnp.dot(rows, up_w, preferred_element_type=jnp.float32)
        inner = (jax.nn.silu(first) * second).astype(jnp.bfloat16)
        out_rows = jnp.dot(inner, down_w, preferred_element_type=jnp.float32).astype(jnp.bfloat16)
        weight = jnp.take(flat_gates, pair_idx, mode='fill', fill_value=0)
        carry = carry.at[token_idx].add(weight[:, None] * out_rows.astype(jnp.float32), mode='drop')
        return carry, None

    windows = pair_for_slot.reshape(EXPERTS, EXPERT_CAP)
    return lax.scan(expert_body, jnp.zeros((TOKENS, D), jnp.float32), (g_weight, u_weight, d_weight, windows))[0]


def reference(hidden, k_cache, v_cache, lengths, w_query, w_key, w_value, w_out, w_router, expert_ids, w_gate, w_up, w_down):
    blocks = TOKENS // ATT_BLOCK

    def layer_step(state, layer):
        cache_k, cache_v, q_weight, k_weight, v_weight, o_weight, r_weight, layer_ids, g_weight, u_weight, d_weight = layer
        normed = rms_norm(state)
        query = jnp.dot(normed, q_weight, preferred_element_type=jnp.float32).astype(jnp.bfloat16)
        key_new = jnp.dot(normed, k_weight, preferred_element_type=jnp.float32).astype(jnp.bfloat16)
        value_new = jnp.dot(normed, v_weight, preferred_element_type=jnp.float32).astype(jnp.bfloat16)
        mixed = lax.map(attend_block, (
            query.reshape(blocks, ATT_BLOCK, KV_HEADS, PER_KV, HEAD),
            cache_k.reshape(blocks, ATT_BLOCK, SEQ_LEN, KV_HEADS, HEAD),
            cache_v.reshape(blocks, ATT_BLOCK, SEQ_LEN, KV_HEADS, HEAD),
            lengths.reshape(blocks, ATT_BLOCK),
            key_new.reshape(blocks, ATT_BLOCK, KV_HEADS, HEAD),
            value_new.reshape(blocks, ATT_BLOCK, KV_HEADS, HEAD)))
        mixed = mixed.reshape(TOKENS, HEADS * HEAD)
        residual = (state.astype(jnp.float32) + jnp.dot(mixed, o_weight, preferred_element_type=jnp.float32)).astype(jnp.bfloat16)
        routed = rms_norm(residual)
        logits = jnp.dot(routed.astype(jnp.float32), r_weight, preferred_element_type=jnp.float32)
        gates = jax.nn.softmax(jnp.take_along_axis(logits, layer_ids, axis=1), axis=-1)
        combined = expert_mix(routed, layer_ids, gates, g_weight, u_weight, d_weight)
        return (residual.astype(jnp.float32) + combined).astype(jnp.bfloat16), None

    layer_inputs = (k_cache, v_cache, w_query, w_key, w_value, w_out, w_router, expert_ids, w_gate, w_up, w_down)
    return lax.scan(layer_step, hidden, layer_inputs)[0]
```

```python
import functools

import jax
import jax.numpy as jnp
from jax import lax
from jax.experimental import pallas as pl
from jax.experimental.pallas import tpu as pltpu
from jax.sharding import PartitionSpec as P

EPS = 1e-6
GROUP_AXES = ('pool', 'ep')
BATCH_AXES = ('dp', 'pool', 'ep')
MESH = pl.DeviceIdType.MESH
F32 = jnp.float32
BF16 = jnp.bfloat16
VMEM_LIMIT = 66_000_000

NZ, NY = 4, 2
GROUP = 16
TOK = 128
HALF = TOK // 2
D = 896
HEADS, KV, HD, SEQ = 16, 4, 128, 32
PER_KV = HEADS // KV
TOP = 8
EXPERTS, LOCAL, FF = 256, 16, 256
SLOTS = LOCAL * TOK
BLK = 16


def rms(wide):
    return wide * lax.rsqrt(jnp.mean(wide * wide, axis=-1, keepdims=True) + EPS)


def dot(a, b):
    return jnp.dot(a, b, preferred_element_type=F32)


def split3(wide):
    high = wide.astype(BF16)
    rest = wide - high.astype(F32)
    mid = rest.astype(BF16)
    low = (rest - mid.astype(F32)).astype(BF16)
    return high, mid, low


def attention_kernel(layer, x_ref, kc_hbm, vc_hbm, len_ref, wq_hbm, wk_hbm, wv_hbm, wo_hbm, wr_hbm, ids_ref,
                     a_ref, u_ref, gate_ref,
                     wq, wk, wv, wo, wr, kc, vc, qs, ks, vs, os, mixed, wsem, ksem, vsem):
    parts = 4
    step = TOK // parts
    loads = [pltpu.make_async_copy(src.at[layer], dst, wsem.at[i]) for i, (src, dst) in enumerate(
        ((wq_hbm, wq), (wk_hbm, wk), (wv_hbm, wv), (wo_hbm, wo), (wr_hbm, wr)))]
    k_loads = [pltpu.make_async_copy(kc_hbm.at[layer, pl.ds(i * step, step)], kc.at[pl.ds(i * step, step)], ksem.at[i]) for i in range(parts)]
    v_loads = [pltpu.make_async_copy(vc_hbm.at[layer, pl.ds(i * step, step)], vc.at[pl.ds(i * step, step)], vsem.at[i]) for i in range(parts)]
    for copy in loads[:3]:
        copy.start()
    for i in range(parts):
        k_loads[i].start()
        v_loads[i].start()
    for copy in loads[3:]:
        copy.start()

    x = x_ref[...].astype(F32)
    h = rms(x).astype(BF16)
    loads[0].wait()
    for c in range(4):
        q = dot(h, wq[:, c * 512:(c + 1) * 512]).astype(BF16).astype(F32)
        for j in range(4):
            qs[pl.ds(c * 4 + j, TOK, stride=HEADS), :] = q[:, j * HD:(j + 1) * HD]
    loads[1].wait()
    k_new = dot(h, wk[...]).astype(BF16).astype(F32)
    loads[2].wait()
    v_new = dot(h, wv[...]).astype(BF16).astype(F32)
    for i in range(HEADS):
        j = i // PER_KV
        ks[pl.ds(i, TOK, stride=HEADS), :] = k_new[:, j * HD:(j + 1) * HD]
        vs[pl.ds(i, TOK, stride=HEADS), :] = v_new[:, j * HD:(j + 1) * HD]

    scale = HD ** -0.5
    lane = lax.broadcasted_iota(jnp.int32, (HEADS, SEQ * KV), 1)
    head = lax.broadcasted_iota(jnp.int32, (HEADS, SEQ * KV), 0)
    own_kv = lax.rem(lane, KV) == head // PER_KV
    pos = jnp.where(own_kv, lane // KV, SEQ)

    def attend(b, carry):
        tok = b * BLK
        rows = pl.ds(tok * HEADS, BLK * HEADS)
        q_wide = qs[rows, :]
        q_blk = q_wide.astype(BF16)
        score_list, mask_list = [], []
        for t in range(BLK):
            score_list.append(lax.dot_general(q_blk[t * HEADS:(t + 1) * HEADS], kc[tok + t], (((1,), (1,)), ((), ())), preferred_element_type=F32))
            mask_list.append(pos < len_ref[0, tok + t])
        score = jnp.concatenate(score_list, axis=0) * scale
        mask = jnp.concatenate(mask_list, axis=0)
        score = jnp.where(mask, score, -jnp.inf)
        score_new = jnp.sum(q_wide * ks[rows, :], axis=-1, keepdims=True) * scale
        peak = jnp.maximum(jnp.max(score, axis=-1, keepdims=True), score_new)
        prob = jnp.exp(score - peak)
        prob_new = jnp.exp(score_new - peak)
        total = jnp.sum(prob, axis=-1, keepdims=True) + prob_new
        prob = (prob / total).astype(BF16)
        prob_new = (prob_new / total).astype(BF16).astype(F32)
        out = [dot(prob[t * HEADS:(t + 1) * HEADS], vc[tok + t]) for t in range(BLK)]
        out = jnp.concatenate(out, axis=0) + prob_new * vs[rows, :]
        os[rows, :] = out.astype(BF16).astype(F32)
        return carry

    per_part = step // BLK
    for i in range(parts):
        k_loads[i].wait()
        v_loads[i].wait()
        lax.fori_loop(i * per_part, (i + 1) * per_part, attend, 0)

    for i in range(HEADS):
        mixed[:, i * HD:(i + 1) * HD] = os[pl.ds(i, TOK, stride=HEADS), :].astype(BF16)
    loads[3].wait()
    a = (x + dot(mixed[...], wo[...])).astype(BF16)
    a_ref[...] = a
    u = rms(a.astype(F32)).astype(BF16)
    u_ref[...] = u
    loads[4].wait()
    high, mid, low = split3(wr[...])
    logits = (dot(u, low) + dot(u, mid)) + dot(u, high)
    logits = logits.T
    expert = lax.broadcasted_iota(jnp.int32, (EXPERTS, TOK), 0)
    chosen = [jnp.sum(jnp.where(expert == ids_ref[layer, k:k + 1, :], logits, 0.0), axis=0, keepdims=True) for k in range(TOP)]
    chosen = jnp.concatenate(chosen, axis=0)
    weight = jnp.exp(chosen - jnp.max(chosen, axis=0, keepdims=True))
    gate_ref[...] = weight / jnp.sum(weight, axis=0, keepdims=True)


def attention(layer, hidden, kc, vc, lengths, wq, wk, wv, wo, wr, ids):
    vmem = pl.BlockSpec(memory_space=pltpu.VMEM)
    hbm = pl.BlockSpec(memory_space=pl.ANY)
    return pl.pallas_call(
        functools.partial(attention_kernel, layer),
        out_shape=(jax.ShapeDtypeStruct((TOK, D), BF16), jax.ShapeDtypeStruct((TOK, D), BF16), jax.ShapeDtypeStruct((TOP, TOK), F32)),
        in_specs=[vmem, hbm, hbm, pl.BlockSpec(memory_space=pltpu.SMEM), hbm, hbm, hbm, hbm, hbm, vmem],
        out_specs=(vmem, vmem, vmem),
        scratch_shapes=[
            pltpu.VMEM((D, HEADS * HD), BF16), pltpu.VMEM((D, KV * HD), BF16), pltpu.VMEM((D, KV * HD), BF16),
            pltpu.VMEM((HEADS * HD, D), BF16), pltpu.VMEM((D, EXPERTS), F32),
            pltpu.VMEM((TOK, SEQ * KV, HD), BF16), pltpu.VMEM((TOK, SEQ * KV, HD), BF16),
            pltpu.VMEM((TOK * HEADS, HD), F32), pltpu.VMEM((TOK * HEADS, HD), F32), pltpu.VMEM((TOK * HEADS, HD), F32),
            pltpu.VMEM((TOK * HEADS, HD), F32), pltpu.VMEM((TOK, HEADS * HD), BF16),
            pltpu.SemaphoreType.DMA((5,)), pltpu.SemaphoreType.DMA((4,)), pltpu.SemaphoreType.DMA((4,)),
        ],
        compiler_params=pltpu.CompilerParams(vmem_limit_bytes=VMEM_LIMIT),
        name='attention',
    )(hidden, kc, vc, lengths, wq, wk, wv, wo, wr, ids)


def remote(src, dst, send, recv, target):
    return pltpu.make_async_remote_copy(src_ref=src, dst_ref=dst, send_sem=send, recv_sem=recv, device_id=target, device_id_type=MESH)


def moe_kernel(layer, u_ref, gate_ref, ids_ref, a_ref, wg_hbm, wu_hbm, wd_hbm, out_ref,
               wg, wu, wd, rows, gates, pos, jpos, tgt, xs, ys, pick,
               own_part, far_part, core_in, y_in, right_in, left_in,
               wsem, gsem_s, gsem_r, az_s, az_r, ay_s, ay_r, ac_s, ac_r,
               rc_s, rc_r, ry_s, ry_r, rr_s, rr_r, rl_s, rl_r):
    z = lax.axis_index('pool')
    ep = lax.axis_index('ep')
    y = ep // 2
    core = lax.rem(ep, 2)

    def at(zz, dy, dc):
        return {'pool': zz, 'ep': lax.rem(y + dy, 2) * 2 + lax.rem(core + dc, 2)}

    def slot(zz, dy, dc):
        return (zz * 2 + dy) * 2 + dc

    barrier = pltpu.get_barrier_semaphore()
    others = [(dz, dy, dc) for dz in range(NZ) for dy in range(NY) for dc in range(2) if (dz, dy, dc) != (0, 0, 0)]
    for dz, dy, dc in others:
        pl.semaphore_signal(barrier, inc=1, device_id=at(lax.rem(z + dz, NZ), dy, dc), device_id_type=MESH)

    chunk = 4
    weights = []
    for i in range(LOCAL // chunk):
        part = pl.ds(i * chunk, chunk)
        for j, (src, dst) in enumerate(((wg_hbm, wg), (wu_hbm, wu), (wd_hbm, wd))):
            weights.append(pltpu.make_async_copy(src.at[layer, part], dst.at[part], wsem.at[j, i]))
    for copy in weights:
        copy.start()

    pl.semaphore_wait(barrier, len(others))

    def block(zz, dy, dc, half):
        return rows.at[zz * 2 + dy, pl.ds(dc * TOK + half * HALF, HALF)]

    def own(half):
        return u_ref.at[pl.ds(half * HALF, HALF)]

    def to_z(zz, half, step):
        src = block(zz, 0, 0, half)
        return remote(src, src, az_s.at[zz, half, (step + 1) // 2], az_r.at[zz, half], at(z + step, 0, 0))

    def own_to_z(half, step):
        return remote(own(half), block(z, 0, 0, half), az_s.at[z, half, (step + 1) // 2], az_r.at[z, half], at(z + step, 0, 0))

    def to_y(zz, half):
        return remote(block(zz, 0, 0, half), block(zz, 1, 0, half), ay_s.at[zz, half], ay_r.at[zz, half], at(z, 1, 0))

    def own_to_y(half):
        return remote(own(half), block(z, 1, 0, half), ay_s.at[z, half], ay_r.at[z, half], at(z, 1, 0))

    def whole(zz, dy, dc):
        return rows.at[zz * 2 + dy, pl.ds(dc * TOK, TOK)]

    def to_core(zz, dy):
        return remote(whole(zz, dy, 0), whole(zz, dy, 1), ac_s.at[zz, dy], ac_r.at[zz, dy], at(z, 0, 1))

    def own_to_core():
        return remote(u_ref, whole(z, 0, 1), ac_s.at[z, 0], ac_r.at[z, 0], at(z, 0, 1))

    own_to_core().start()
    for half in range(2):
        @pl.when(z < NZ - 1)
        def _():
            own_to_z(half, 1).start()

        @pl.when(z > 0)
        def _():
            own_to_z(half, -1).start()
        own_to_y(half).start()

    def gate_copy(dz, dy, dc):
        me = slot(z, dy, dc)
        return remote(gate_ref, gates.at[me], gsem_s.at[dz * 4 + dy * 2 + dc], gsem_r.at[me], at(lax.rem(z + dz, NZ), dy, dc))

    for o in others:
        gate_copy(*o).start()
    gates[slot(z, 0, 0)] = gate_ref[...]
    rows[z * 2, pl.ds(0, TOK), :] = u_ref[...]

    first = (z * 4 + ep) * LOCAL
    expert = lax.broadcasted_iota(jnp.int32, (LOCAL, TOK), 0) + first
    tri = (lax.broadcasted_iota(jnp.int32, (TOK, TOK), 0) < lax.broadcasted_iota(jnp.int32, (TOK, TOK), 1)).astype(BF16)
    ones = jnp.ones((TOK, TOK), BF16)
    low = (lax.broadcasted_iota(jnp.int32, (LOCAL, LOCAL), 1) < lax.broadcasted_iota(jnp.int32, (LOCAL, LOCAL), 0)).astype(BF16)
    lane = lax.broadcasted_iota(jnp.int32, (LOCAL, TOK), 1).astype(F32)

    def source(s):
        zz = s // 4
        dy = lax.rem(s // 2, 2)
        dc = lax.rem(s, 2)
        return zz * 4 + lax.rem(y + dy, 2) * 2 + lax.rem(core + dc, 2)

    def plan(s, base):
        ids = ids_ref[source(s)]
        hit = jnp.zeros((LOCAL, TOK), F32)
        for k in range(TOP):
            hit = hit + jnp.where(expert == ids[k:k + 1, :], 1.0, 0.0)
        hit16 = hit.astype(BF16)
        rank = dot(hit16, tri)
        count = dot(hit16, ones)
        offset = dot(low, count.astype(BF16))
        pos[s] = jnp.where(hit > 0, base + rank, -1.0)
        jpos[s] = jnp.where(hit > 0, offset + rank, -1.0)
        local = lane - base
        tgt[s] = jnp.where((local >= 0) & (local < count), local + offset, -1.0)
        return base + count

    lax.fori_loop(0, GROUP, plan, jnp.zeros((LOCAL, TOK), F32))

    sub = lax.broadcasted_iota(jnp.int32, (TOK, TOK), 0).astype(F32)

    def fill(zz, dy, fresh):
        chip = zz * 2 + dy

        def body(e2, carry):
            picks = []
            for j in range(2):
                e = e2 * 2 + j
                picks.append(jnp.concatenate([(sub == pos[chip * 2 + dc, pl.ds(e, 1), :]).astype(F32).astype(BF16) for dc in range(2)], axis=1))
            got = dot(jnp.concatenate(picks, axis=0), rows[chip])
            where = pl.ds(pl.multiple_of(e2 * 2 * TOK, 2 * TOK), 2 * TOK)
            if fresh:
                xs[where, :] = got
            else:
                xs[where, :] += got
            return carry
        lax.fori_loop(0, LOCAL // 2, body, 0)

    def arrive(zz, step):
        last = (z == NZ - 1) if step == 1 else (z == 0)
        for half in range(2):
            remote(block(zz, 0, 0, half), block(zz, 0, 0, half), az_s.at[zz, half, 0], az_r.at[zz, half], at(z, 0, 1)).wait_recv()

            @pl.when(jnp.logical_not(last))
            def _():
                to_z(zz, half, step).start()
            to_y(zz, half).start()
        to_core(zz, 0).start()

    def core_recv(zz, dy):
        to_core(zz, dy).wait_recv()

    def y_recv(zz):
        for half in range(2):
            to_y(zz, half).wait_recv()
        to_core(zz, 1).start()

    core_recv(z, 0)
    fill(z, 0, True)

    for k in range(1, NZ):
        @pl.when(z - k >= 0)
        def _():
            arrive(z - k, 1)

        @pl.when(z + k < NZ)
        def _():
            arrive(z + k, -1)
        if k == 1:
            y_recv(z)

        @pl.when(z - k >= 0)
        def _():
            core_recv(z - k, 0)
            fill(z - k, 0, False)

        @pl.when(z + k < NZ)
        def _():
            core_recv(z + k, 0)
            fill(z + k, 0, False)
        if k == 1:
            core_recv(z, 1)
            fill(z, 1, False)
    for k in range(1, NZ):
        zz = lax.rem(z + k, NZ)
        y_recv(zz)
        core_recv(zz, 1)
        fill(zz, 1, False)

    def experts(e, carry):
        window = pl.ds(pl.multiple_of(e * TOK, TOK), TOK)
        x = xs[window, :].astype(BF16)
        inner = (jax.nn.silu(dot(x, wg[e])) * dot(x, wu[e])).astype(BF16)
        ys[window, :] = dot(inner, wd[e]).astype(BF16)
        return carry
    for i in range(LOCAL // chunk):
        for copy in weights[3 * i:3 * i + 3]:
            copy.wait()
        lax.fori_loop(i * chunk, (i + 1) * chunk, experts, 0)

    for dz, dy, dc in others:
        gate_copy(dz, dy, dc).wait_send()
        s = slot(lax.rem(z + dz, NZ), dy, dc)
        remote(gate_ref, gates.at[s], gsem_s.at[0], gsem_r.at[s], at(z, 0, 1)).wait_recv()

    side = z // 2
    near = z - side * (2 * z - 3)
    order = []
    for i in range(NZ):
        value = (3, 2, 1 - near, near)[i]
        order.append(value + side * (3 - 2 * value))

    def weighted(s):
        ids = ids_ref[source(s)]
        gate = gates[s]
        g = jnp.zeros((LOCAL, TOK), F32)
        for k in range(TOP):
            g = g + jnp.where(expert == ids[k:k + 1, :], gate[k:k + 1, :], 0.0)
        jp = jpos[s]
        acc = jnp.zeros((TOK, TOK), F32)
        for e in range(LOCAL):
            acc = acc + jnp.where(sub == jp[e:e + 1, :], g[e:e + 1, :], 0.0)
        return split3(acc.T)

    def core_copy(zd, dy):
        i = zd * 2 + dy
        return remote(far_part.at[i], core_in.at[i], rc_s.at[i], rc_r.at[i], at(z, 0, 1))

    def y_copy(zd, half):
        part = pl.ds(half * HALF, HALF)
        return remote(own_part.at[zd * 2 + 1, part], y_in.at[zd, part], ry_s.at[zd, half], ry_r.at[zd, half], at(z, 1, 0))

    def z_copy(zd, half, step):
        part = pl.ds(half * HALF, HALF)
        if step == 1:
            return remote(own_part.at[zd * 2, part], right_in.at[zd, part], rr_s.at[zd, half], rr_r.at[zd, half], at(z + 1, 0, 0))
        return remote(own_part.at[zd * 2, part], left_in.at[zd, part], rl_s.at[zd, half], rl_r.at[zd, half], at(z - 1, 0, 0))

    def z_wait(zd, half, step):
        part = pl.ds(half * HALF, HALF)
        if step == 1:
            remote(own_part.at[zd * 2, part], right_in.at[zd, part], rr_s.at[zd, half], rr_r.at[zd, half], at(z, 0, 1)).wait_recv()
        else:
            remote(own_part.at[zd * 2, part], left_in.at[zd, part], rl_s.at[zd, half], rl_r.at[zd, half], at(z, 0, 1)).wait_recv()

    def combine(i, carry):
        value = jnp.where(i == 0, order[0], jnp.where(i == 1, order[1], jnp.where(i == 2, order[2], order[3])))
        zd = value
        for dy in (1, 0):
            s = slot(zd, dy, 0)
            for r in range(2):
                for e in range(LOCAL):
                    pick[r * TOK:(r + 1) * TOK, e * TOK:(e + 1) * TOK] = (sub == tgt[s + 1 - r, e:e + 1, :]).astype(F32).astype(BF16)
            pairs = dot(pick[...], ys[...]).astype(BF16)
            for r, part in ((0, far_part), (1, own_part)):
                high, mid, low3 = weighted(s + 1 - r)
                mine = pairs[r * TOK:(r + 1) * TOK]
                part[zd * 2 + dy] = (dot(low3, mine) + dot(mid, mine)) + dot(high, mine)
                if r == 0:
                    core_copy(zd, dy).start()
        for dy in (1, 0):
            core_copy(zd, dy).wait_recv()
            for half in range(2):
                part = pl.ds(half * HALF, HALF)
                own_part[zd * 2 + dy, part] += core_in[zd * 2 + dy, part]
                if dy == 1:
                    y_copy(zd, half).start()
        return carry

    lax.fori_loop(0, NZ, combine, 0)

    for i in range(NZ):
        zd = order[i]
        for half in range(2):
            part = pl.ds(half * HALF, HALF)
            y_copy(zd, half).wait_recv()
            own_part[zd * 2, part] += y_in[zd, part]
            if i < NZ - 1:
                @pl.when(zd > z)
                def _():
                    @pl.when(z > 0)
                    def _():
                        z_wait(zd, half, 1)
                        own_part[zd * 2, part] += right_in[zd, part]
                    z_copy(zd, half, 1).start()

                @pl.when(zd < z)
                def _():
                    @pl.when(z < NZ - 1)
                    def _():
                        z_wait(zd, half, -1)
                        own_part[zd * 2, part] += left_in[zd, part]
                    z_copy(zd, half, -1).start()
            else:
                @pl.when(z > 0)
                def _():
                    z_wait(z, half, 1)
                    own_part[z * 2, part] += right_in[z, part]

                @pl.when(z < NZ - 1)
                def _():
                    z_wait(z, half, -1)
                    own_part[z * 2, part] += left_in[z, part]
                out_ref[part, :] = (a_ref[part, :].astype(F32) + own_part[z * 2, part]).astype(BF16)

    own_to_core().wait_send()
    for half in range(2):
        own_to_y(half).wait_send()

        @pl.when(z < NZ - 1)
        def _():
            own_to_z(half, 1).wait_send()

        @pl.when(z > 0)
        def _():
            own_to_z(half, -1).wait_send()
    for k in range(1, NZ):
        zz = lax.rem(z + k, NZ)
        to_core(zz, 0).wait_send()
        for half in range(2):
            to_y(zz, half).wait_send()

            @pl.when((zz < z) & (z < NZ - 1))
            def _():
                to_z(zz, half, 1).wait_send()

            @pl.when((zz > z) & (z > 0))
            def _():
                to_z(zz, half, -1).wait_send()
    for zz in range(NZ):
        to_core(zz, 1).wait_send()
        for dy in range(2):
            core_copy(zz, dy).wait_send()
        for half in range(2):
            y_copy(zz, half).wait_send()

            @pl.when(zz > z)
            def _():
                z_copy(zz, half, 1).wait_send()

            @pl.when(zz < z)
            def _():
                z_copy(zz, half, -1).wait_send()


def moe(layer, u, gates, ids_all, a, wg, wu, wd):
    vmem = pl.BlockSpec(memory_space=pltpu.VMEM)
    hbm = pl.BlockSpec(memory_space=pl.ANY)
    sem = pltpu.SemaphoreType.DMA
    return pl.pallas_call(
        functools.partial(moe_kernel, layer),
        out_shape=jax.ShapeDtypeStruct((TOK, D), BF16),
        in_specs=[vmem, vmem, vmem, vmem, hbm, hbm, hbm],
        out_specs=vmem,
        scratch_shapes=[
            pltpu.VMEM((LOCAL, D, FF), BF16), pltpu.VMEM((LOCAL, D, FF), BF16), pltpu.VMEM((LOCAL, FF, D), BF16),
            pltpu.VMEM((NZ * NY, 2 * TOK, D), BF16), pltpu.VMEM((GROUP, TOP, TOK), F32),
            pltpu.VMEM((GROUP, LOCAL, TOK), F32), pltpu.VMEM((GROUP, LOCAL, TOK), F32), pltpu.VMEM((GROUP, LOCAL, TOK), F32),
            pltpu.VMEM((SLOTS, D), F32), pltpu.VMEM((SLOTS, D), BF16), pltpu.VMEM((2 * TOK, SLOTS), BF16),
            pltpu.VMEM((NZ * NY, TOK, D), F32), pltpu.VMEM((NZ * NY, TOK, D), F32), pltpu.VMEM((NZ * NY, TOK, D), F32),
            pltpu.VMEM((NZ, TOK, D), F32), pltpu.VMEM((NZ, TOK, D), F32), pltpu.VMEM((NZ, TOK, D), F32),
            sem((3, 4)), sem((GROUP,)), sem((GROUP,)),
            sem((NZ, 2, 2)), sem((NZ, 2)), sem((NZ, 2)), sem((NZ, 2)), sem((NZ, 2)), sem((NZ, 2)),
            sem((NZ * NY,)), sem((NZ * NY,)), sem((NZ, 2)), sem((NZ, 2)), sem((NZ, 2)), sem((NZ, 2)), sem((NZ, 2)), sem((NZ, 2)),
        ],
        compiler_params=pltpu.CompilerParams(vmem_limit_bytes=VMEM_LIMIT, collective_id=layer, has_side_effects=True),
        name='moe',
    )(u, gates, ids_all, a, wg, wu, wd)


def solution(mesh):
    def device_step(hidden, k_cache, v_cache, lengths, w_query, w_key, w_value, w_out, w_router, expert_ids, w_gate, w_up, w_down):
        layers = expert_ids.shape[0]
        kc = k_cache.reshape(layers, TOK, SEQ * KV, HD)
        vc = v_cache.reshape(layers, TOK, SEQ * KV, HD)
        ids = jnp.swapaxes(expert_ids, 1, 2)
        ids_all = lax.all_gather(ids, GROUP_AXES)
        for layer in range(layers):
            a, u, gates = attention(layer, hidden, kc, vc, lengths[None], w_query, w_key, w_value, w_out, w_router, ids)
            hidden = moe(layer, u, gates, ids_all[:, layer], a, w_gate, w_up, w_down)
        return hidden

    cache_spec = P(None, BATCH_AXES, None, None, None)
    expert_spec = P(None, GROUP_AXES, None, None)
    in_specs = (P(BATCH_AXES, None), cache_spec, cache_spec, P(BATCH_AXES), P(), P(), P(), P(), P(), P(None, BATCH_AXES, None), expert_spec, expert_spec, expert_spec)
    return jax.shard_map(device_step, mesh=mesh, in_specs=in_specs, out_specs=P(BATCH_AXES, None), check_vma=False)
```

```python
import functools

import jax
import jax.numpy as jnp
from jax import lax
from jax.experimental import pallas as pl
from jax.experimental.pallas import tpu as pltpu
from jax.sharding import PartitionSpec as P

EPS = 1e-6
GROUP_AXES = ('pool', 'ep')
BATCH_AXES = ('dp', 'pool', 'ep')
MESH = pl.DeviceIdType.MESH
F32 = jnp.float32
BF16 = jnp.bfloat16
VMEM_LIMIT = 66_000_000

NZ, NY = 4, 2
GROUP = 16
TOK = 128
HALF = TOK // 2
D = 896
HEADS, KV, HD, SEQ = 16, 4, 128, 32
PER_KV = HEADS // KV
TOP = 8
EXPERTS, LOCAL, FF = 256, 16, 256
SLOTS = LOCAL * TOK
BLK = 16


def rms(wide):
    return wide * lax.rsqrt(jnp.mean(wide * wide, axis=-1, keepdims=True) + EPS)


def dot(a, b):
    return jnp.dot(a, b, preferred_element_type=F32)


def split3(wide):
    high = wide.astype(BF16)
    rest = wide - high.astype(F32)
    mid = rest.astype(BF16)
    low = (rest - mid.astype(F32)).astype(BF16)
    return high, mid, low


OTHERS = [(dz, dy, dc) for dz in range(NZ) for dy in range(NY) for dc in range(2) if (dz, dy, dc) != (0, 0, 0)]


def position():
    z = lax.axis_index('pool')
    ep = lax.axis_index('ep')
    y = ep // 2
    core = lax.rem(ep, 2)

    def at(zz, dy, dc):
        return {'pool': zz, 'ep': lax.rem(y + dy, 2) * 2 + lax.rem(core + dc, 2)}
    return z, y, core, at


def slot(zz, dy, dc):
    return (zz * 2 + dy) * 2 + dc


def remote(src, dst, send, recv, target):
    return pltpu.make_async_remote_copy(src_ref=src, dst_ref=dst, send_sem=send, recv_sem=recv, device_id=target, device_id_type=MESH)


def attention_kernel(layer, x_ref, kc_hbm, vc_hbm, len_ref, wq_hbm, wk_hbm, wv_hbm, wo_hbm, wr_hbm, ids_ref, *refs):
    share = layer == 0
    if share:
        a_ref, u_ref, gate_ref, all_ref, wq, wk, wv, wo, wr, kc, vc, qs, ks, vs, os, mixed, wsem, ksem, vsem, held, send_sem, recv_sem = refs
    else:
        a_ref, u_ref, gate_ref, wq, wk, wv, wo, wr, kc, vc, qs, ks, vs, os, mixed, wsem, ksem, vsem = refs
    if share:
        z, y, core, at = position()
        barrier = pltpu.get_barrier_semaphore()
        for dz, dy, dc in OTHERS:
            pl.semaphore_signal(barrier, inc=1, device_id=at(lax.rem(z + dz, NZ), dy, dc), device_id_type=MESH)
    parts = 4
    step = TOK // parts
    loads = [pltpu.make_async_copy(src.at[layer], dst, wsem.at[i]) for i, (src, dst) in enumerate(
        ((wq_hbm, wq), (wk_hbm, wk), (wv_hbm, wv), (wo_hbm, wo), (wr_hbm, wr)))]
    k_loads = [pltpu.make_async_copy(kc_hbm.at[layer, pl.ds(i * step, step)], kc.at[pl.ds(i * step, step)], ksem.at[i]) for i in range(parts)]
    v_loads = [pltpu.make_async_copy(vc_hbm.at[layer, pl.ds(i * step, step)], vc.at[pl.ds(i * step, step)], vsem.at[i]) for i in range(parts)]
    for copy in loads[:3]:
        copy.start()
    for i in range(parts):
        k_loads[i].start()
        v_loads[i].start()
    for copy in loads[3:]:
        copy.start()
    if share:
        pl.semaphore_wait(barrier, len(OTHERS))
        sends = []
        for dz, dy, dc in OTHERS:
            sends.append(remote(ids_ref, held.at[slot(z, dy, dc)], send_sem.at[dz * 4 + dy * 2 + dc], recv_sem.at[slot(z, dy, dc)], at(lax.rem(z + dz, NZ), dy, dc)))
            sends[-1].start()
        held[slot(z, 0, 0)] = ids_ref[...]

    x = x_ref[...].astype(F32)
    h = rms(x).astype(BF16)
    loads[0].wait()
    for c in range(4):
        q = dot(h, wq[:, c * 512:(c + 1) * 512]).astype(BF16).astype(F32)
        for j in range(4):
            qs[pl.ds(c * 4 + j, TOK, stride=HEADS), :] = q[:, j * HD:(j + 1) * HD]
    loads[1].wait()
    k_new = dot(h, wk[...]).astype(BF16).astype(F32)
    loads[2].wait()
    v_new = dot(h, wv[...]).astype(BF16).astype(F32)
    for i in range(HEADS):
        j = i // PER_KV
        ks[pl.ds(i, TOK, stride=HEADS), :] = k_new[:, j * HD:(j + 1) * HD]
        vs[pl.ds(i, TOK, stride=HEADS), :] = v_new[:, j * HD:(j + 1) * HD]

    scale = HD ** -0.5
    lane = lax.broadcasted_iota(jnp.int32, (HEADS, SEQ * KV), 1)
    head = lax.broadcasted_iota(jnp.int32, (HEADS, SEQ * KV), 0)
    own_kv = lax.rem(lane, KV) == head // PER_KV
    pos = jnp.where(own_kv, lane // KV, SEQ)

    def attend(b, carry):
        tok = b * BLK
        rows = pl.ds(tok * HEADS, BLK * HEADS)
        q_wide = qs[rows, :]
        q_blk = q_wide.astype(BF16)
        score_list, mask_list = [], []
        for t in range(BLK):
            score_list.append(lax.dot_general(q_blk[t * HEADS:(t + 1) * HEADS], kc[tok + t], (((1,), (1,)), ((), ())), preferred_element_type=F32))
            mask_list.append(pos < len_ref[0, tok + t])
        score = jnp.concatenate(score_list, axis=0) * scale
        mask = jnp.concatenate(mask_list, axis=0)
        score = jnp.where(mask, score, -jnp.inf)
        score_new = jnp.sum(q_wide * ks[rows, :], axis=-1, keepdims=True) * scale
        peak = jnp.maximum(jnp.max(score, axis=-1, keepdims=True), score_new)
        prob = jnp.exp(score - peak)
        prob_new = jnp.exp(score_new - peak)
        total = jnp.sum(prob, axis=-1, keepdims=True) + prob_new
        prob = (prob / total).astype(BF16)
        prob_new = (prob_new / total).astype(BF16).astype(F32)
        out = [dot(prob[t * HEADS:(t + 1) * HEADS], vc[tok + t]) for t in range(BLK)]
        out = jnp.concatenate(out, axis=0) + prob_new * vs[rows, :]
        os[rows, :] = out.astype(BF16).astype(F32)
        return carry

    per_part = step // BLK
    for i in range(parts):
        k_loads[i].wait()
        v_loads[i].wait()
        lax.fori_loop(i * per_part, (i + 1) * per_part, attend, 0)

    for i in range(HEADS):
        mixed[:, i * HD:(i + 1) * HD] = os[pl.ds(i, TOK, stride=HEADS), :].astype(BF16)
    loads[3].wait()
    a = (x + dot(mixed[...], wo[...])).astype(BF16)
    a_ref[...] = a
    u = rms(a.astype(F32)).astype(BF16)
    u_ref[...] = u
    loads[4].wait()
    high, mid, low = split3(wr[...])
    logits = (dot(u, low) + dot(u, mid)) + dot(u, high)
    logits = logits.T
    expert = lax.broadcasted_iota(jnp.int32, (EXPERTS, TOK), 0)
    chosen = [jnp.sum(jnp.where(expert == ids_ref[layer, k:k + 1, :], logits, 0.0), axis=0, keepdims=True) for k in range(TOP)]
    chosen = jnp.concatenate(chosen, axis=0)
    weight = jnp.exp(chosen - jnp.max(chosen, axis=0, keepdims=True))
    gate_ref[...] = weight / jnp.sum(weight, axis=0, keepdims=True)
    if share:
        for copy, (dz, dy, dc) in zip(sends, OTHERS):
            i = slot(lax.rem(z + dz, NZ), dy, dc)
            copy.wait_send()
            remote(ids_ref, held.at[i], send_sem.at[0], recv_sem.at[i], at(z, 0, 1)).wait_recv()
        all_ref[...] = held[...]


def attention(layer, hidden, kc, vc, lengths, wq, wk, wv, wo, wr, ids):
    vmem = pl.BlockSpec(memory_space=pltpu.VMEM)
    hbm = pl.BlockSpec(memory_space=pl.ANY)
    out_shape = (jax.ShapeDtypeStruct((TOK, D), BF16), jax.ShapeDtypeStruct((TOK, D), BF16), jax.ShapeDtypeStruct((TOP, TOK), F32))
    params = dict(vmem_limit_bytes=VMEM_LIMIT)
    extra = []
    if layer == 0:
        out_shape += (jax.ShapeDtypeStruct((GROUP,) + ids.shape, jnp.int32),)
        extra = [pltpu.VMEM((GROUP,) + ids.shape, jnp.int32), pltpu.SemaphoreType.DMA((GROUP,)), pltpu.SemaphoreType.DMA((GROUP,))]
        params.update(collective_id=2, has_side_effects=True)
    return pl.pallas_call(
        functools.partial(attention_kernel, layer),
        out_shape=out_shape,
        in_specs=[vmem, hbm, hbm, pl.BlockSpec(memory_space=pltpu.SMEM), hbm, hbm, hbm, hbm, hbm, vmem],
        out_specs=(vmem,) * len(out_shape),
        scratch_shapes=[
            pltpu.VMEM((D, HEADS * HD), BF16), pltpu.VMEM((D, KV * HD), BF16), pltpu.VMEM((D, KV * HD), BF16),
            pltpu.VMEM((HEADS * HD, D), BF16), pltpu.VMEM((D, EXPERTS), F32),
            pltpu.VMEM((TOK, SEQ * KV, HD), BF16), pltpu.VMEM((TOK, SEQ * KV, HD), BF16),
            pltpu.VMEM((TOK * HEADS, HD), F32), pltpu.VMEM((TOK * HEADS, HD), F32), pltpu.VMEM((TOK * HEADS, HD), F32),
            pltpu.VMEM((TOK * HEADS, HD), F32), pltpu.VMEM((TOK, HEADS * HD), BF16),
            pltpu.SemaphoreType.DMA((5,)), pltpu.SemaphoreType.DMA((4,)), pltpu.SemaphoreType.DMA((4,)),
        ] + extra,
        compiler_params=pltpu.CompilerParams(**params),
        name='attention',
    )(hidden, kc, vc, lengths, wq, wk, wv, wo, wr, ids)


EDGE = 16
GATHER = ((0, 80), (80, 48))
REDUCE = ((0, EDGE), (EDGE, 56), (72, 56))


def moe_kernel(layer, u_ref, gate_ref, ids_ref, a_ref, wg_hbm, wu_hbm, wd_hbm, out_ref,
               wg, wu, wd, rows, gates, pos, jpos, tgt, xs, ys, pick,
               core_in, y_in, y_edge, right_in, right_edge, left_in, left_edge,
               wsem, gsem_s, gsem_r, az_s, az_r, ay_s, ay_r, ac_s, ac_r,
               rc_s, rc_r, ry_s, ry_r, rr_s, rr_r, rl_s, rl_r):
    z, y, core, at = position()
    first = (z * 4 + y * 2 + core) * LOCAL
    side = z // 2
    near = z - side * (2 * z - 3)
    mirror = lambda v: v + side * (3 - 2 * v)
    n1, n2, n3 = mirror(1 - near), mirror(2), mirror(3)
    order = (mirror(3), mirror(2), mirror(1 - near), mirror(near))

    barrier = pltpu.get_barrier_semaphore()
    for dz, dy, dc in OTHERS:
        pl.semaphore_signal(barrier, inc=1, device_id=at(lax.rem(z + dz, NZ), dy, dc), device_id_type=MESH)

    chunk = 4
    weights = []
    for i in range(LOCAL // chunk):
        part = pl.ds(i * chunk, chunk)
        for j, (src, dst) in enumerate(((wg_hbm, wg), (wu_hbm, wu), (wd_hbm, wd))):
            weights.append(pltpu.make_async_copy(src.at[layer, part], dst.at[part], wsem.at[j, i]))
    for copy in weights:
        copy.start()

    expert = lax.broadcasted_iota(jnp.int32, (LOCAL, TOK), 0) + first
    tri = (lax.broadcasted_iota(jnp.int32, (TOK, TOK), 0) < lax.broadcasted_iota(jnp.int32, (TOK, TOK), 1)).astype(BF16)
    ones = jnp.ones((TOK, TOK), BF16)
    low = (lax.broadcasted_iota(jnp.int32, (LOCAL, LOCAL), 1) < lax.broadcasted_iota(jnp.int32, (LOCAL, LOCAL), 0)).astype(BF16)
    lane = lax.broadcasted_iota(jnp.int32, (LOCAL, TOK), 1).astype(F32)
    sub = lax.broadcasted_iota(jnp.int32, (TOK, TOK), 0).astype(F32)

    def plan(s, base):
        ids = ids_ref[s, layer]
        hit = jnp.zeros((LOCAL, TOK), F32)
        for k in range(TOP):
            hit = hit + jnp.where(expert == ids[k:k + 1, :], 1.0, 0.0)
        hit16 = hit.astype(BF16)
        rank = dot(hit16, tri)
        count = dot(hit16, ones)
        offset = dot(low, count.astype(BF16))
        pos[s] = jnp.where(hit > 0, base + rank, -1.0)
        jpos[s] = jnp.where(hit > 0, offset + rank, -1.0)
        local = lane - base
        tgt[s] = jnp.where((local >= 0) & (local < count), local + offset, -1.0)
        return base + count

    with jax.named_scope('plan'):
        lax.fori_loop(0, GROUP, plan, jnp.zeros((LOCAL, TOK), F32), unroll=2)

    with jax.named_scope('barrier'):
        pl.semaphore_wait(barrier, len(OTHERS))

    def block(zz, dy, dc, start, count):
        return rows.at[zz * 2 + dy, pl.ds(dc * TOK + start, count)]

    def z_send(zz, c, step):
        if c == 2:
            src = block(zz, 1, 0, 0, EDGE)
        else:
            src = block(zz, 0, 0, *GATHER[c])
        return remote(src, src, az_s.at[zz, c, (step + 1) // 2], az_r.at[zz, c], at(z + step, 0, 0))

    def own_z_send(c, step):
        return remote(u_ref.at[pl.ds(*GATHER[c])], block(z, 0, 0, *GATHER[c]), az_s.at[z, c, (step + 1) // 2], az_r.at[z, c], at(z + step, 0, 0))

    def z_arrival(zz, c):
        src = block(zz, 1, 0, 0, EDGE) if c == 2 else block(zz, 0, 0, *GATHER[c])
        return remote(src, src, az_s.at[zz, c, 0], az_r.at[zz, c], at(z, 0, 1))

    def y_piece(c):
        start, count = GATHER[c]
        return (EDGE, count - EDGE) if c == 0 else (start, count)

    def y_send(zz, c):
        return remote(block(zz, 0, 0, *y_piece(c)), block(zz, 1, 0, *y_piece(c)), ay_s.at[zz, c], ay_r.at[zz, c], at(z, 1, 0))

    def own_y_send(c):
        return remote(u_ref.at[pl.ds(*GATHER[c])], block(z, 1, 0, *GATHER[c]), ay_s.at[z, c], ay_r.at[z, c], at(z, 1, 0))

    def core_send(zz, dy):
        return remote(block(zz, dy, 0, 0, TOK), block(zz, dy, 1, 0, TOK), ac_s.at[zz, dy], ac_r.at[zz, dy], at(z, 0, 1))

    def own_core_send():
        return remote(u_ref, block(z, 0, 1, 0, TOK), ac_s.at[z, 0], ac_r.at[z, 0], at(z, 0, 1))

    def both_ways(make, act):
        @pl.when(z < NZ - 1)
        def _():
            getattr(make(1), act)()

        @pl.when(z > 0)
        def _():
            getattr(make(-1), act)()

    def onward(zz, c, act):
        @pl.when((zz < z) & (z < NZ - 1))
        def _():
            getattr(z_send(zz, c, 1), act)()

        @pl.when((zz > z) & (z > 0))
        def _():
            getattr(z_send(zz, c, -1), act)()

    own_core_send().start()
    for c in range(2):
        both_ways(lambda step: own_z_send(c, step), 'start')
        own_y_send(c).start()

    def gate_copy(dz, dy, dc):
        me = slot(z, dy, dc)
        return remote(gate_ref, gates.at[me], gsem_s.at[dz * 4 + dy * 2 + dc], gsem_r.at[me], at(lax.rem(z + dz, NZ), dy, dc))

    for o in OTHERS:
        gate_copy(*o).start()
    gates[slot(z, 0, 0)] = gate_ref[...]
    rows[z * 2, pl.ds(0, TOK), :] = u_ref[...]

    per = 4

    def fill(zz, dy, fresh=False):
        chip = zz * 2 + dy

        def body(i, carry):
            picks = []
            for j in range(per):
                e = i * per + j
                picks.append(jnp.concatenate([(sub == pos[chip * 2 + dc, pl.ds(e, 1), :]).astype(F32).astype(BF16) for dc in range(2)], axis=1))
            got = dot(jnp.concatenate(picks, axis=0), rows[chip])
            where = pl.ds(pl.multiple_of(i * per * TOK, per * TOK), per * TOK)
            if fresh:
                xs[where, :] = got
            else:
                xs[where, :] += got
            return carry
        with jax.named_scope('fill'):
            core_send(zz, dy).wait_recv()
            lax.fori_loop(0, LOCAL // per, body, 0)

    def arrive(zz, c):
        z_arrival(zz, c).wait_recv()
        onward(zz, c, 'start')
        if c < 2:
            y_send(zz, c).start()
        if c == 1:
            core_send(zz, 0).start()

    def arrive_y(zz):
        for c in range(2):
            y_send(zz, c).wait_recv()
        core_send(zz, 1).start()

    inside, end = near == 1, near == 0
    fill(z, 0, True)
    arrive(n1, 0)
    pl.when(inside)(lambda: arrive(n2, 0))
    own_y_send(0).wait_recv()
    both_ways(lambda step: z_send(z, 2, step), 'start')
    arrive(n1, 1)
    pl.when(inside)(lambda: arrive(n2, 1))
    own_y_send(1).wait_recv()
    core_send(z, 1).start()
    fill(n1, 0)
    pl.when(end)(lambda: arrive(n2, 0))
    pl.when(inside)(lambda: arrive(n3, 0))
    arrive(n1, 2)
    pl.when(inside)(lambda: arrive(n2, 2))
    fill(z, 1)
    pl.when(end)(lambda: arrive(n2, 1))
    pl.when(inside)(lambda: arrive(n3, 1))
    fill(n2, 0)
    pl.when(end)(lambda: arrive(n2, 2))
    pl.when(end)(lambda: arrive(n3, 0))
    arrive_y(n1)
    fill(n1, 1)
    pl.when(end)(lambda: arrive(n3, 1))
    arrive_y(n2)
    fill(n3, 0)
    arrive(n3, 2)
    fill(n2, 1)
    arrive_y(n3)
    fill(n3, 1)

    def experts(e, carry):
        window = pl.ds(pl.multiple_of(e * TOK, TOK), TOK)
        x = xs[window, :].astype(BF16)
        inner = (jax.nn.silu(dot(x, wg[e])) * dot(x, wu[e])).astype(BF16)
        ys[window, :] = dot(inner, wd[e]).astype(BF16)
        return carry
    with jax.named_scope('experts'):
        for i in range(LOCAL // chunk):
            for copy in weights[3 * i:3 * i + 3]:
                copy.wait()
            lax.fori_loop(i * chunk, (i + 1) * chunk, experts, 0)

    for dz, dy, dc in OTHERS:
        gate_copy(dz, dy, dc).wait_send()
        s = slot(lax.rem(z + dz, NZ), dy, dc)
        remote(gate_ref, gates.at[s], gsem_s.at[0], gsem_r.at[s], at(z, 0, 1)).wait_recv()

    def own_part(i, start=0, count=TOK):
        return xs.at[pl.ds(pl.multiple_of(i * TOK + start, 8), count)]

    def far_part(i):
        return xs.at[pl.ds(pl.multiple_of((NZ * NY + i) * TOK, TOK), TOK)]

    def weighted(s):
        ids = ids_ref[s, layer]
        gate = gates[s]
        g = jnp.zeros((LOCAL, TOK), F32)
        for k in range(TOP):
            g = g + jnp.where(expert == ids[k:k + 1, :], gate[k:k + 1, :], 0.0)
        jp = jpos[s]
        acc = jnp.zeros((TOK, TOK), F32)
        for e in range(LOCAL):
            acc = acc + jnp.where(sub == jp[e:e + 1, :], g[e:e + 1, :], 0.0)
        return split3(acc.T)

    def core_copy(i):
        return remote(far_part(i), core_in.at[i], rc_s.at[i], rc_r.at[i], at(z, 0, 1))

    def y_copy(zd, c):
        part = pl.ds(*REDUCE[c])
        if c == 0:
            dst = y_edge
        else:
            dst = y_in.at[zd, part]
        return remote(own_part(zd * 2 + 1, *REDUCE[c]), dst, ry_s.at[zd, c], ry_r.at[zd, c], at(z, 1, 0))

    def z_copy(zd, c, step, target=None):
        main, edge, send, recv = (right_in, right_edge, rr_s, rr_r) if step == 1 else (left_in, left_edge, rl_s, rl_r)
        target = at(z + step, 0, 0) if target is None else target
        if c == 3:
            return remote(own_part(zd * 2 + 1, 0, EDGE), edge.at[zd], send.at[zd, c], recv.at[zd, c], target)
        return remote(own_part(zd * 2, *REDUCE[c]), main.at[zd, pl.ds(*REDUCE[c])], send.at[zd, c], recv.at[zd, c], target)

    def take(zd, c, step):
        z_copy(zd, c, step, at(z, 0, 1)).wait_recv()
        main, edge = (right_in, right_edge) if step == 1 else (left_in, left_edge)
        if c == 3:
            own_part(zd * 2 + 1, 0, EDGE)[...] += edge[zd]
        else:
            own_part(zd * 2, *REDUCE[c])[...] += main[zd, pl.ds(*REDUCE[c])]

    def chain(zd, c):
        @pl.when(zd > z)
        def _():
            @pl.when(z > 0)
            def _():
                take(zd, c, 1)
            z_copy(zd, c, 1).start()

        @pl.when(zd < z)
        def _():
            @pl.when(z < NZ - 1)
            def _():
                take(zd, c, -1)
            z_copy(zd, c, -1).start()

    def last(c):
        @pl.when(z > 0)
        def _():
            take(z, c, 1)

        @pl.when(z < NZ - 1)
        def _():
            take(z, c, -1)

    def cross(zd, c):
        y_copy(zd, c).wait_recv()
        own_part(zd * 2, *REDUCE[c])[...] += y_in[zd, pl.ds(*REDUCE[c])]

    def edges(zd):
        chain(zd, 0)
        chain(zd, 3)

    def piece(zd, c):
        cross(zd, c)
        chain(zd, c)

    steps = ((0, 1), (1, 1), (0, 0), (2, 1), (1, 0), (3, 1), (2, 0), (3, 0))
    targets = [order[i] * 2 + dy for i, dy in steps]

    def pick_target(j):
        value = targets[0]
        for i in range(1, len(steps)):
            value = jnp.where(j == i, targets[i], value)
        return value

    def finish(j):
        i = pick_target(j)
        core_copy(i).wait_recv()
        own_part(i)[...] += core_in[i]

        @pl.when(lax.rem(i, 2) == 1)
        def _():
            for c in (1, 2):
                y_copy(i // 2, c).start()

    def combine(j, carry):
        i = pick_target(j)
        s = i * 2
        for r in range(2):
            for e in range(LOCAL):
                pick[r * TOK:(r + 1) * TOK, e * TOK:(e + 1) * TOK] = (sub == tgt[s + 1 - r, e:e + 1, :]).astype(F32).astype(BF16)
        pairs = dot(pick[...], ys[...]).astype(BF16)
        for r, part in ((0, far_part), (1, own_part)):
            high, mid, low3 = weighted(s + 1 - r)
            mine = pairs[r * TOK:(r + 1) * TOK]
            part(i)[...] = (dot(low3, mine) + dot(mid, mine)) + dot(high, mine)
            if r == 0:
                core_copy(i).start()

        @pl.when(j > 0)
        def _():
            finish(j - 1)

        @pl.when(end & (j == 4))
        def _():
            edges(order[0])
            piece(order[0], 1)

        @pl.when(end & (j == 5))
        def _():
            piece(order[0], 2)

        @pl.when(end & (j == 7))
        def _():
            edges(order[1])
            piece(order[1], 1)
        return carry

    with jax.named_scope('combine'):
        lax.fori_loop(0, len(steps), combine, 0)

    with jax.named_scope('chain'):
        finish(len(steps) - 1)

        @pl.when(inside)
        def _():
            edges(order[0])
            piece(order[0], 1)
            piece(order[0], 2)
            edges(order[1])
            piece(order[1], 1)
        piece(order[1], 2)
        edges(order[2])
        piece(order[2], 1)
        last(3)
        y_copy(z, 0).start()
        piece(order[2], 2)
        last(0)
        for c in (1, 2):
            cross(z, c)
            last(c)
        y_copy(z, 0).wait_recv()
        own_part(z * 2, 0, EDGE)[...] += y_edge[...]
        out_ref[...] = (a_ref[...].astype(F32) + own_part(z * 2)[...]).astype(BF16)

    own_core_send().wait_send()
    for c in range(2):
        own_y_send(c).wait_send()
        both_ways(lambda step: own_z_send(c, step), 'wait_send')
    both_ways(lambda step: z_send(z, 2, step), 'wait_send')
    for zz in (n1, n2, n3):
        core_send(zz, 0).wait_send()
        for c in range(3):
            onward(zz, c, 'wait_send')
            if c < 2:
                y_send(zz, c).wait_send()
    for zz in range(NZ):
        core_send(zz, 1).wait_send()
        for dy in range(2):
            core_copy(zz * 2 + dy).wait_send()
        for c in (1, 2):
            y_copy(zz, c).wait_send()
        for c in range(4):
            @pl.when(zz > z)
            def _():
                z_copy(zz, c, 1).wait_send()

            @pl.when(zz < z)
            def _():
                z_copy(zz, c, -1).wait_send()
    y_copy(z, 0).wait_send()


def moe(layer, u, gates, ids_all, a, wg, wu, wd):
    vmem = pl.BlockSpec(memory_space=pltpu.VMEM)
    hbm = pl.BlockSpec(memory_space=pl.ANY)
    sem = pltpu.SemaphoreType.DMA
    return pl.pallas_call(
        functools.partial(moe_kernel, layer),
        out_shape=jax.ShapeDtypeStruct((TOK, D), BF16),
        in_specs=[vmem, vmem, vmem, vmem, hbm, hbm, hbm],
        out_specs=vmem,
        scratch_shapes=[
            pltpu.VMEM((LOCAL, D, FF), BF16), pltpu.VMEM((LOCAL, D, FF), BF16), pltpu.VMEM((LOCAL, FF, D), BF16),
            pltpu.VMEM((NZ * NY, 2 * TOK, D), BF16), pltpu.VMEM((GROUP, TOP, TOK), F32),
            pltpu.VMEM((GROUP, LOCAL, TOK), F32), pltpu.VMEM((GROUP, LOCAL, TOK), F32), pltpu.VMEM((GROUP, LOCAL, TOK), F32),
            pltpu.VMEM((SLOTS, D), F32), pltpu.VMEM((SLOTS, D), BF16), pltpu.VMEM((2 * TOK, SLOTS), BF16),
            pltpu.VMEM((NZ * NY, TOK, D), F32), pltpu.VMEM((NZ, TOK, D), F32), pltpu.VMEM((EDGE, D), F32),
            pltpu.VMEM((NZ, TOK, D), F32), pltpu.VMEM((NZ, EDGE, D), F32), pltpu.VMEM((NZ, TOK, D), F32), pltpu.VMEM((NZ, EDGE, D), F32),
            sem((3, 4)), sem((GROUP,)), sem((GROUP,)),
            sem((NZ, 3, 2)), sem((NZ, 3)), sem((NZ, 2)), sem((NZ, 2)), sem((NZ, 2)), sem((NZ, 2)),
            sem((NZ * NY,)), sem((NZ * NY,)), sem((NZ, 3)), sem((NZ, 3)), sem((NZ, 4)), sem((NZ, 4)), sem((NZ, 4)), sem((NZ, 4)),
        ],
        compiler_params=pltpu.CompilerParams(vmem_limit_bytes=VMEM_LIMIT, collective_id=layer, has_side_effects=True),
        name='moe',
    )(u, gates, ids_all, a, wg, wu, wd)


def solution(mesh):
    def device_step(hidden, k_cache, v_cache, lengths, w_query, w_key, w_value, w_out, w_router, expert_ids, w_gate, w_up, w_down):
        layers = expert_ids.shape[0]
        kc = k_cache.reshape(layers, TOK, SEQ * KV, HD)
        vc = v_cache.reshape(layers, TOK, SEQ * KV, HD)
        ids = jnp.swapaxes(expert_ids, 1, 2)
        for layer in range(layers):
            a, u, gates, *shared = attention(layer, hidden, kc, vc, lengths[None], w_query, w_key, w_value, w_out, w_router, ids)
            if shared:
                ids_all = shared[0]
            hidden = moe(layer, u, gates, ids_all, a, w_gate, w_up, w_down)
        return hidden

    cache_spec = P(None, BATCH_AXES, None, None, None)
    expert_spec = P(None, GROUP_AXES, None, None)
    in_specs = (P(BATCH_AXES, None), cache_spec, cache_spec, P(BATCH_AXES), P(), P(), P(), P(), P(), P(None, BATCH_AXES, None), expert_spec, expert_spec, expert_spec)
    return jax.shard_map(device_step, mesh=mesh, in_specs=in_specs, out_specs=P(BATCH_AXES, None), check_vma=False)
```

```python
import functools

import jax
import jax.numpy as jnp
from jax import lax
from jax.experimental import pallas as pl
from jax.experimental.pallas import tpu as pltpu
from jax.sharding import PartitionSpec as P

EPS = 1e-6
GROUP_AXES = ('pool', 'ep')
BATCH_AXES = ('dp', 'pool', 'ep')
MESH = pl.DeviceIdType.MESH
F32 = jnp.float32
BF16 = jnp.bfloat16
VMEM_LIMIT = 66_000_000

NZ, NY = 4, 2
GROUP = 16
TOK = 128
HALF = TOK // 2
D = 896
HEADS, KV, HD, SEQ = 16, 4, 128, 32
PER_KV = HEADS // KV
TOP = 8
EXPERTS, LOCAL, FF = 256, 16, 256
SLOTS = LOCAL * TOK
BLK = 16


def rms(wide):
    return wide * lax.rsqrt(jnp.mean(wide * wide, axis=-1, keepdims=True) + EPS)


def dot(a, b):
    return jnp.dot(a, b, preferred_element_type=F32)


def split3(wide):
    high = wide.astype(BF16)
    rest = wide - high.astype(F32)
    mid = rest.astype(BF16)
    low = (rest - mid.astype(F32)).astype(BF16)
    return high, mid, low


OTHERS = [(dz, dy, dc) for dz in range(NZ) for dy in range(NY) for dc in range(2) if (dz, dy, dc) != (0, 0, 0)]


def position():
    z = lax.axis_index('pool')
    ep = lax.axis_index('ep')
    y = ep // 2
    core = lax.rem(ep, 2)

    def at(zz, dy, dc):
        return {'pool': zz, 'ep': lax.rem(y + dy, 2) * 2 + lax.rem(core + dc, 2)}
    return z, y, core, at


def slot(zz, dy, dc):
    return (zz * 2 + dy) * 2 + dc


def remote(src, dst, send, recv, target):
    return pltpu.make_async_remote_copy(src_ref=src, dst_ref=dst, send_sem=send, recv_sem=recv, device_id=target, device_id_type=MESH)


EDGE = 16
GATHER = ((0, 80), (80, 48))
REDUCE = ((0, EDGE), (EDGE, 56), (72, 56))


def kernel(layers, x_ref, kc_hbm, vc_hbm, len_ref, wq_hbm, wk_hbm, wv_hbm, wo_hbm, wr_hbm, ids_own, wg_hbm, wu_hbm, wd_hbm, out_ref,
           wg, wu, wd, wr, rows, xs, ys, pick, mix, gates, pos, jpos, tgt, base_ref, ids_ref,
           x_s, a_ref, u_ref, gate_ref, qs, ks, vs, mixed,
           core_in, y_in, y_edge, right_in, right_edge, left_in, left_edge,
           wsem, asem, ksem, vsem, isem_s, isem_r, gsem_s, gsem_r, az_s, az_r, ay_s, ay_r, ac_s, ac_r,
           rc_s, rc_r, ry_s, ry_r, rr_s, rr_r, rl_s, rl_r):
    z, y, core, at = position()
    first = (z * 4 + y * 2 + core) * LOCAL
    side = z // 2
    near = z - side * (2 * z - 3)
    mirror = lambda v: v + side * (3 - 2 * v)
    n1, n2, n3 = mirror(1 - near), mirror(2), mirror(3)
    order = (mirror(3), mirror(2), mirror(1 - near), mirror(near))
    inside, end = near == 1, near == 0

    barrier = pltpu.get_barrier_semaphore()
    for dz, dy, dc in OTHERS:
        pl.semaphore_signal(barrier, inc=1, device_id=at(lax.rem(z + dz, NZ), dy, dc), device_id_type=MESH)

    def attention_loads(layer):
        pairs = [(wq_hbm.at[layer, :, pl.ds(c * FF, FF)], wg.at[c]) for c in range(8)]
        pairs += [(wk_hbm.at[layer, :, pl.ds(c * FF, FF)], wg.at[8 + c]) for c in range(2)]
        pairs += [(wv_hbm.at[layer, :, pl.ds(c * FF, FF)], wg.at[10 + c]) for c in range(2)]
        pairs += [(wo_hbm.at[layer, pl.ds(c * FF, FF)], wd.at[c]) for c in range(8)]
        pairs += [(wr_hbm.at[layer], wr)]
        return [pltpu.make_async_copy(src, dst, asem.at[i]) for i, (src, dst) in enumerate(pairs)]

    def cache_loads(layer):
        copies = []
        for hbm, start, sem in ((kc_hbm, 0, ksem), (vc_hbm, TOK // BLK, vsem)):
            for q in range(BLK):
                copies.append(pltpu.make_async_copy(hbm.at[layer, :, q], pick.at[pl.ds(start, TOK // BLK), :, pl.ds(q * HD, HD)], sem.at[q]))
        return copies

    chunk = 4

    def expert_loads(layer):
        copies = []
        for i in range(LOCAL // chunk):
            part = pl.ds(i * chunk, chunk)
            for j, (src, dst) in enumerate(((wg_hbm, wg), (wu_hbm, wu), (wd_hbm, wd))):
                copies.append(pltpu.make_async_copy(src.at[layer, part], dst.at[part], wsem.at[j, i]))
        return copies

    def start(copies):
        for copy in copies:
            copy.start()

    def ids_copy(dz, dy, dc):
        me = slot(z, dy, dc)
        return remote(ids_own, ids_ref.at[me], isem_s.at[dz * 4 + dy * 2 + dc], isem_r.at[me], at(lax.rem(z + dz, NZ), dy, dc))

    def ids_start():
        pl.semaphore_wait(barrier, len(OTHERS))
        for o in OTHERS:
            ids_copy(*o).start()
        ids_ref[slot(z, 0, 0)] = ids_own[...]

    def ids_wait():
        for dz, dy, dc in OTHERS:
            ids_copy(dz, dy, dc).wait_send()
            i = slot(lax.rem(z + dz, NZ), dy, dc)
            remote(ids_own, ids_ref.at[i], isem_s.at[0], isem_r.at[i], at(z, 0, 1)).wait_recv()

    scale = HD ** -0.5
    pair_lane = lax.broadcasted_iota(jnp.int32, (HEADS, SEQ * KV), 1)
    pair_head = lax.broadcasted_iota(jnp.int32, (HEADS, SEQ * KV), 0)
    pair_pos = jnp.where(lax.rem(pair_lane, KV) == pair_head // PER_KV, pair_lane // KV, SEQ)

    def attend(b, carry):
        tok = b * BLK
        part = pl.ds(tok * HEADS, BLK * HEADS)
        q_wide = qs[part, :]
        q_blk = q_wide.astype(BF16)
        score_list, mask_list = [], []
        for t in range(BLK):
            keys = pick[b, :, t * HD:(t + 1) * HD]
            score_list.append(lax.dot_general(q_blk[t * HEADS:(t + 1) * HEADS], keys, (((1,), (1,)), ((), ())), preferred_element_type=F32))
            mask_list.append(pair_pos < len_ref[0, tok + t])
        score = jnp.concatenate(score_list, axis=0) * scale
        mask = jnp.concatenate(mask_list, axis=0)
        score = jnp.where(mask, score, -jnp.inf)
        score_new = jnp.sum(q_wide * ks[part, :], axis=-1, keepdims=True) * scale
        peak = jnp.maximum(jnp.max(score, axis=-1, keepdims=True), score_new)
        prob = jnp.exp(score - peak)
        prob_new = jnp.exp(score_new - peak)
        total = jnp.sum(prob, axis=-1, keepdims=True) + prob_new
        prob = (prob / total).astype(BF16)
        prob_new = (prob_new / total).astype(BF16).astype(F32)
        out = [dot(prob[t * HEADS:(t + 1) * HEADS], pick[TOK // BLK + b, :, t * HD:(t + 1) * HD]) for t in range(BLK)]
        out = jnp.concatenate(out, axis=0) + prob_new * vs[part, :]
        qs[part, :] = out.astype(BF16).astype(F32)
        return carry

    def attention(layer, x_from):
        loads = attention_loads(layer)
        x = x_from[...].astype(F32)
        h = rms(x).astype(BF16)
        with jax.named_scope('qkv'):
            for c in range(8):
                loads[c].wait()
                q = dot(h, wg[c]).astype(BF16).astype(F32)
                for j in range(2):
                    qs[pl.ds(c * 2 + j, TOK, stride=HEADS), :] = q[:, j * HD:(j + 1) * HD]
            for c in range(2):
                loads[8 + c].wait()
                loads[10 + c].wait()
                k_new = dot(h, wg[8 + c]).astype(BF16).astype(F32)
                v_new = dot(h, wg[10 + c]).astype(BF16).astype(F32)
                for i in range(8):
                    j = i // PER_KV
                    ks[pl.ds(c * 8 + i, TOK, stride=HEADS), :] = k_new[:, j * HD:(j + 1) * HD]
                    vs[pl.ds(c * 8 + i, TOK, stride=HEADS), :] = v_new[:, j * HD:(j + 1) * HD]
        if layer == 0:
            with jax.named_scope('barrier'):
                ids_start()
        with jax.named_scope('att'):
            for copy in cache_loads(layer):
                copy.wait()
            lax.fori_loop(0, TOK // BLK, attend, 0)
        with jax.named_scope('post'):
            for i in range(HEADS):
                mixed[:, i * HD:(i + 1) * HD] = qs[pl.ds(i, TOK, stride=HEADS), :].astype(BF16)
            for copy in loads[12:]:
                copy.wait()
            a = (x + dot(mixed[...], wd[0:8].reshape(HEADS * HD, D))).astype(BF16)
            a_ref[...] = a
            u = rms(a.astype(F32)).astype(BF16)
            u_ref[...] = u
            high, mid, low3 = split3(wr[...])
            logits = ((dot(u, low3) + dot(u, mid)) + dot(u, high)).T
            row = lax.broadcasted_iota(jnp.int32, (EXPERTS, TOK), 0)
            chosen = [jnp.sum(jnp.where(row == ids_own[layer, k:k + 1, :], logits, 0.0), axis=0, keepdims=True) for k in range(TOP)]
            chosen = jnp.concatenate(chosen, axis=0)
            weight = jnp.exp(chosen - jnp.max(chosen, axis=0, keepdims=True))
            gate_ref[...] = weight / jnp.sum(weight, axis=0, keepdims=True)

    expert = lax.broadcasted_iota(jnp.int32, (LOCAL, TOK), 0) + first
    tri = (lax.broadcasted_iota(jnp.int32, (TOK, TOK), 0) < lax.broadcasted_iota(jnp.int32, (TOK, TOK), 1)).astype(BF16)
    ones = jnp.ones((TOK, TOK), BF16)
    low = (lax.broadcasted_iota(jnp.int32, (LOCAL, LOCAL), 1) < lax.broadcasted_iota(jnp.int32, (LOCAL, LOCAL), 0)).astype(BF16)
    lane = lax.broadcasted_iota(jnp.int32, (LOCAL, TOK), 1).astype(F32)
    sub = lax.broadcasted_iota(jnp.int32, (TOK, TOK), 0).astype(F32)
    sub16 = sub.astype(BF16)

    def onehot(row):
        row16 = jnp.broadcast_to(row, (16, TOK)).astype(BF16)
        return jnp.where(sub16 == jnp.concatenate([row16] * (TOK // 16), axis=0), jnp.ones((TOK, TOK), BF16), jnp.zeros((TOK, TOK), BF16))

    def plan(layer, s, base):
        ids = ids_ref[s, layer]
        hit = jnp.zeros((LOCAL, TOK), F32)
        for k in range(TOP):
            hit = hit + jnp.where(expert == ids[k:k + 1, :], 1.0, 0.0)
        hit16 = hit.astype(BF16)
        rank = dot(hit16, tri)
        count = dot(hit16, ones)
        offset = dot(low, count.astype(BF16))
        pos[s] = jnp.where(hit > 0, base + rank, -1.0)
        jpos[s] = jnp.where(hit > 0, offset + rank, -1.0)
        local = lane - base
        tgt[s] = jnp.where((local >= 0) & (local < count), local + offset, -1.0)
        return base + count

    def plan_part(layer, begin, stop):
        if begin == 0:
            base_ref[...] = jnp.zeros((LOCAL, TOK), F32)
        base_ref[...] = lax.fori_loop(begin, stop, functools.partial(plan, layer), base_ref[...], unroll=2)

    def block(zz, dy, dc, start, count):
        return rows.at[zz * 2 + dy, pl.ds(dc * TOK + start, count)]

    def z_send(zz, c, step):
        if c == 2:
            src = block(zz, 1, 0, 0, EDGE)
        else:
            src = block(zz, 0, 0, *GATHER[c])
        return remote(src, src, az_s.at[zz, c, (step + 1) // 2], az_r.at[zz, c], at(z + step, 0, 0))

    def own_z_send(c, step):
        return remote(u_ref.at[pl.ds(*GATHER[c])], block(z, 0, 0, *GATHER[c]), az_s.at[z, c, (step + 1) // 2], az_r.at[z, c], at(z + step, 0, 0))

    def z_arrival(zz, c):
        src = block(zz, 1, 0, 0, EDGE) if c == 2 else block(zz, 0, 0, *GATHER[c])
        return remote(src, src, az_s.at[zz, c, 0], az_r.at[zz, c], at(z, 0, 1))

    def y_piece(c):
        start, count = GATHER[c]
        return (EDGE, count - EDGE) if c == 0 else (start, count)

    def y_send(zz, c):
        return remote(block(zz, 0, 0, *y_piece(c)), block(zz, 1, 0, *y_piece(c)), ay_s.at[zz, c], ay_r.at[zz, c], at(z, 1, 0))

    def own_y_send(c):
        return remote(u_ref.at[pl.ds(*GATHER[c])], block(z, 1, 0, *GATHER[c]), ay_s.at[z, c], ay_r.at[z, c], at(z, 1, 0))

    def core_send(zz, dy):
        return remote(block(zz, dy, 0, 0, TOK), block(zz, dy, 1, 0, TOK), ac_s.at[zz, dy], ac_r.at[zz, dy], at(z, 0, 1))

    def own_core_send():
        return remote(u_ref, block(z, 0, 1, 0, TOK), ac_s.at[z, 0], ac_r.at[z, 0], at(z, 0, 1))

    def both_ways(make, act):
        @pl.when(z < NZ - 1)
        def _():
            getattr(make(1), act)()

        @pl.when(z > 0)
        def _():
            getattr(make(-1), act)()

    def onward(zz, c, act):
        @pl.when((zz < z) & (z < NZ - 1))
        def _():
            getattr(z_send(zz, c, 1), act)()

        @pl.when((zz > z) & (z > 0))
        def _():
            getattr(z_send(zz, c, -1), act)()

    def gate_copy(dz, dy, dc):
        me = slot(z, dy, dc)
        return remote(gate_ref, gates.at[me], gsem_s.at[dz * 4 + dy * 2 + dc], gsem_r.at[me], at(lax.rem(z + dz, NZ), dy, dc))

    per = 4

    def fill(zz, dy, fresh=False):
        chip = zz * 2 + dy

        def body(i, carry):
            picks = []
            for j in range(per):
                e = i * per + j
                picks.append(jnp.concatenate([onehot(pos[chip * 2 + dc, pl.ds(e, 1), :]) for dc in range(2)], axis=1))
            got = dot(jnp.concatenate(picks, axis=0), rows[chip])
            where = pl.ds(pl.multiple_of(i * per * TOK, per * TOK), per * TOK)
            if fresh:
                xs[where, :] = got
            else:
                xs[where, :] += got
            return carry
        with jax.named_scope('fill'):
            core_send(zz, dy).wait_recv()
            lax.fori_loop(0, LOCAL // per, body, 0)

    def arrive(zz, c):
        z_arrival(zz, c).wait_recv()
        onward(zz, c, 'start')
        if c < 2:
            y_send(zz, c).start()
        if c == 1:
            core_send(zz, 0).start()

    def arrive_y(zz):
        for c in range(2):
            y_send(zz, c).wait_recv()
        core_send(zz, 1).start()

    def gather(layer):
        own_core_send().start()
        for c in range(2):
            both_ways(lambda step: own_z_send(c, step), 'start')
            own_y_send(c).start()

        for o in OTHERS:
            gate_copy(*o).start()
        gates[slot(z, 0, 0)] = gate_ref[...]
        rows[z * 2, pl.ds(0, TOK), :] = u_ref[...]

        start(expert_loads(layer))
        if layer == 0:
            with jax.named_scope('plan'):
                ids_wait()
                plan_part(0, 0, GROUP)
        fill(z, 0, True)
        arrive(n1, 0)
        pl.when(inside)(lambda: arrive(n2, 0))
        own_y_send(0).wait_recv()
        both_ways(lambda step: z_send(z, 2, step), 'start')
        arrive(n1, 1)
        pl.when(inside)(lambda: arrive(n2, 1))
        own_y_send(1).wait_recv()
        core_send(z, 1).start()
        fill(n1, 0)
        pl.when(end)(lambda: arrive(n2, 0))
        pl.when(inside)(lambda: arrive(n3, 0))
        arrive(n1, 2)
        pl.when(inside)(lambda: arrive(n2, 2))
        fill(z, 1)
        pl.when(end)(lambda: arrive(n2, 1))
        pl.when(inside)(lambda: arrive(n3, 1))
        fill(n2, 0)
        pl.when(end)(lambda: arrive(n2, 2))
        pl.when(end)(lambda: arrive(n3, 0))
        arrive_y(n1)
        fill(n1, 1)
        pl.when(end)(lambda: arrive(n3, 1))
        arrive_y(n2)
        fill(n3, 0)
        arrive(n3, 2)
        fill(n2, 1)
        arrive_y(n3)
        fill(n3, 1)

        own_core_send().wait_send()
        for c in range(2):
            own_y_send(c).wait_send()
            both_ways(lambda step: own_z_send(c, step), 'wait_send')
        both_ways(lambda step: z_send(z, 2, step), 'wait_send')
        for zz in (n1, n2, n3):
            core_send(zz, 0).wait_send()
            for c in range(3):
                onward(zz, c, 'wait_send')
                if c < 2:
                    y_send(zz, c).wait_send()
        for zz in range(NZ):
            core_send(zz, 1).wait_send()
        for dz, dy, dc in OTHERS:
            gate_copy(dz, dy, dc).wait_send()
            s = slot(lax.rem(z + dz, NZ), dy, dc)
            remote(gate_ref, gates.at[s], gsem_s.at[0], gsem_r.at[s], at(z, 0, 1)).wait_recv()

    def ready(layer, s):
        ids = ids_ref[s, layer]
        gate = gates[s]
        g = jnp.zeros((LOCAL, TOK), F32)
        for k in range(TOP):
            g = g + jnp.where(expert == ids[k:k + 1, :], gate[k:k + 1, :], 0.0)
        jp = jpos[s]
        acc = jnp.zeros((TOK, TOK), F32)
        for e in range(LOCAL):
            acc = acc + jnp.where(sub == jp[e:e + 1, :], g[e:e + 1, :], 0.0)
        for i, part in enumerate(split3(acc.T)):
            mix[s, i * TOK:(i + 1) * TOK, :] = part
        for e in range(LOCAL):
            pick[s, :, e * TOK:(e + 1) * TOK] = onehot(tgt[s, e:e + 1, :])

    def experts(layer, e, carry):
        ready(layer, e)
        window = pl.ds(pl.multiple_of(e * TOK, TOK), TOK)
        x = xs[window, :].astype(BF16)
        inner = (jax.nn.silu(dot(x, wg[e])) * dot(x, wu[e])).astype(BF16)
        ys[window, :] = dot(inner, wd[e]).astype(BF16)
        return carry
    def all_experts(layer):
        with jax.named_scope('experts'):
            weights = expert_loads(layer)
            for i in range(LOCAL // chunk):
                for copy in weights[3 * i:3 * i + 3]:
                    copy.wait()
                lax.fori_loop(i * chunk, (i + 1) * chunk, functools.partial(experts, layer), 0)

    def own_part(i, start=0, count=TOK):
        return xs.at[pl.ds(pl.multiple_of(i * TOK + start, 8), count)]

    def far_part(i):
        return xs.at[pl.ds(pl.multiple_of((NZ * NY + i) * TOK, TOK), TOK)]

    def core_copy(i):
        return remote(far_part(i), core_in.at[i], rc_s.at[i], rc_r.at[i], at(z, 0, 1))

    def y_copy(zd, c):
        part = pl.ds(*REDUCE[c])
        if c == 0:
            dst = y_edge
        else:
            dst = y_in.at[zd, part]
        return remote(own_part(zd * 2 + 1, *REDUCE[c]), dst, ry_s.at[zd, c], ry_r.at[zd, c], at(z, 1, 0))

    def z_copy(zd, c, step, target=None):
        main, edge, send, recv = (right_in, right_edge, rr_s, rr_r) if step == 1 else (left_in, left_edge, rl_s, rl_r)
        target = at(z + step, 0, 0) if target is None else target
        if c == 3:
            return remote(own_part(zd * 2 + 1, 0, EDGE), edge.at[zd], send.at[zd, c], recv.at[zd, c], target)
        return remote(own_part(zd * 2, *REDUCE[c]), main.at[zd, pl.ds(*REDUCE[c])], send.at[zd, c], recv.at[zd, c], target)

    def take(zd, c, step):
        z_copy(zd, c, step, at(z, 0, 1)).wait_recv()
        main, edge = (right_in, right_edge) if step == 1 else (left_in, left_edge)
        if c == 3:
            own_part(zd * 2 + 1, 0, EDGE)[...] += edge[zd]
        else:
            own_part(zd * 2, *REDUCE[c])[...] += main[zd, pl.ds(*REDUCE[c])]

    def chain(zd, c):
        @pl.when(zd > z)
        def _():
            @pl.when(z > 0)
            def _():
                take(zd, c, 1)
            z_copy(zd, c, 1).start()

        @pl.when(zd < z)
        def _():
            @pl.when(z < NZ - 1)
            def _():
                take(zd, c, -1)
            z_copy(zd, c, -1).start()

    def last(c):
        @pl.when(z > 0)
        def _():
            take(z, c, 1)

        @pl.when(z < NZ - 1)
        def _():
            take(z, c, -1)

    def cross(zd, c):
        y_copy(zd, c).wait_recv()
        own_part(zd * 2, *REDUCE[c])[...] += y_in[zd, pl.ds(*REDUCE[c])]

    def edges(zd):
        chain(zd, 0)
        chain(zd, 3)

    def piece(zd, c):
        cross(zd, c)
        chain(zd, c)

    targets = [order[i] * 2 + dy for i in range(NZ) for dy in (1, 0)]

    def pick_target(j):
        value = targets[0]
        for i in range(1, len(targets)):
            value = jnp.where(j == i, targets[i], value)
        return value

    def finish(j):
        i = pick_target(j)
        core_copy(i).wait_recv()
        own_part(i)[...] += core_in[i]

        @pl.when(lax.rem(i, 2) == 1)
        def _():
            for c in (1, 2):
                y_copy(i // 2, c).start()

    def combine(j, carry):
        i = pick_target(j)
        s = i * 2
        pairs = dot(pick[pl.ds(s, 2)].reshape(2 * TOK, SLOTS), ys[...]).astype(BF16)
        for dc, part in ((1, far_part), (0, own_part)):
            got = dot(mix[s + dc], pairs[dc * TOK:(dc + 1) * TOK])
            part(i)[...] = (got[2 * TOK:] + got[TOK:2 * TOK]) + got[:TOK]
            if dc == 1:
                core_copy(i).start()

        @pl.when(j > 0)
        def _():
            finish(j - 1)

        @pl.when(end & (j == 2))
        def _():
            edges(order[0])

        @pl.when(end & (j == 4))
        def _():
            edges(order[1])

        @pl.when(end & (j == 5))
        def _():
            piece(order[0], 1)

        @pl.when(end & (j == 7))
        def _():
            piece(order[0], 2)

        @pl.when(inside & (j == 5))
        def _():
            edges(order[0])

        @pl.when(inside & (j == 7))
        def _():
            edges(order[1])
        return carry

    def reduce(layer):
        def ahead(i):
            if layer + 1 < layers:
                plan_part(layer + 1, i * 4, i * 4 + 4)

        with jax.named_scope('combine'):
            lax.fori_loop(0, len(targets), combine, 0)
        if layer + 1 < layers:
            start(cache_loads(layer + 1))

        with jax.named_scope('chain'):
            finish(len(targets) - 1)

            edges(order[2])

            @pl.when(inside)
            def _():
                piece(order[0], 1)
            ahead(0)

            @pl.when(inside)
            def _():
                piece(order[0], 2)
            ahead(1)
            piece(order[1], 1)
            ahead(2)
            piece(order[1], 2)
            last(3)
            y_copy(z, 0).start()
            ahead(3)
            piece(order[2], 1)
            piece(order[2], 2)
            last(0)
            for c in (1, 2):
                cross(z, c)
                last(c)
            y_copy(z, 0).wait_recv()
            own_part(z * 2, 0, EDGE)[...] += y_edge[...]
            dest = x_s if layer + 1 < layers else out_ref
            dest[...] = (a_ref[...].astype(F32) + own_part(z * 2)[...]).astype(BF16)

        for zz in range(NZ):
            for dy in range(2):
                core_copy(zz * 2 + dy).wait_send()
            for c in (1, 2):
                y_copy(zz, c).wait_send()
            for c in range(4):
                @pl.when(zz > z)
                def _():
                    z_copy(zz, c, 1).wait_send()

                @pl.when(zz < z)
                def _():
                    z_copy(zz, c, -1).wait_send()
        y_copy(z, 0).wait_send()


    start(attention_loads(0))
    start(cache_loads(0))
    for layer in range(layers):
        attention(layer, x_ref if layer == 0 else x_s)
        gather(layer)
        all_experts(layer)
        if layer + 1 < layers:
            start(attention_loads(layer + 1))
        reduce(layer)


def solution(mesh):
    def device_step(hidden, k_cache, v_cache, lengths, w_query, w_key, w_value, w_out, w_router, expert_ids, w_gate, w_up, w_down):
        layers = expert_ids.shape[0]
        kc = k_cache.reshape(layers, TOK // BLK, BLK, SEQ * KV, HD)
        vc = v_cache.reshape(layers, TOK // BLK, BLK, SEQ * KV, HD)
        ids = jnp.swapaxes(expert_ids, 1, 2)
        vmem = pl.BlockSpec(memory_space=pltpu.VMEM)
        hbm = pl.BlockSpec(memory_space=pl.ANY)
        sem = pltpu.SemaphoreType.DMA
        buf = pltpu.VMEM
        return pl.pallas_call(
            functools.partial(kernel, layers),
            out_shape=jax.ShapeDtypeStruct((TOK, D), BF16),
            in_specs=[vmem, hbm, hbm, pl.BlockSpec(memory_space=pltpu.SMEM), hbm, hbm, hbm, hbm, hbm, vmem, hbm, hbm, hbm],
            out_specs=vmem,
            scratch_shapes=[
                buf((LOCAL, D, FF), BF16), buf((LOCAL, D, FF), BF16), buf((LOCAL, FF, D), BF16), buf((D, EXPERTS), F32),
                buf((NZ * NY, 2 * TOK, D), BF16), buf((SLOTS, D), F32), buf((SLOTS, D), BF16), buf((GROUP, TOK, SLOTS), BF16), buf((GROUP, 3 * TOK, TOK), BF16),
                buf((GROUP, TOP, TOK), F32), buf((GROUP, LOCAL, TOK), F32), buf((GROUP, LOCAL, TOK), F32), buf((GROUP, LOCAL, TOK), F32),
                buf((LOCAL, TOK), F32), buf((GROUP,) + ids.shape, jnp.int32),
                buf((TOK, D), BF16), buf((TOK, D), BF16), buf((TOK, D), BF16), buf((TOP, TOK), F32),
                buf((TOK * HEADS, HD), F32), buf((TOK * HEADS, HD), F32), buf((TOK * HEADS, HD), F32), buf((TOK, HEADS * HD), BF16),
                buf((NZ * NY, TOK, D), F32), buf((NZ, TOK, D), F32), buf((EDGE, D), F32),
                buf((NZ, TOK, D), F32), buf((NZ, EDGE, D), F32), buf((NZ, TOK, D), F32), buf((NZ, EDGE, D), F32),
                sem((3, 4)), sem((21,)), sem((BLK,)), sem((BLK,)), sem((GROUP,)), sem((GROUP,)), sem((GROUP,)), sem((GROUP,)),
                sem((NZ, 3, 2)), sem((NZ, 3)), sem((NZ, 2)), sem((NZ, 2)), sem((NZ, 2)), sem((NZ, 2)),
                sem((NZ * NY,)), sem((NZ * NY,)), sem((NZ, 3)), sem((NZ, 3)), sem((NZ, 4)), sem((NZ, 4)), sem((NZ, 4)), sem((NZ, 4)),
            ],
            compiler_params=pltpu.CompilerParams(vmem_limit_bytes=67_043_328, collective_id=0, has_side_effects=True),
            name='layers',
        )(hidden, kc, vc, lengths[None], w_query, w_key, w_value, w_out, w_router, ids, w_gate, w_up, w_down)

    cache_spec = P(None, BATCH_AXES, None, None, None)
    expert_spec = P(None, GROUP_AXES, None, None)
    in_specs = (P(BATCH_AXES, None), cache_spec, cache_spec, P(BATCH_AXES), P(), P(), P(), P(), P(), P(None, BATCH_AXES, None), expert_spec, expert_spec, expert_spec)
    return jax.shard_map(device_step, mesh=mesh, in_specs=in_specs, out_specs=P(BATCH_AXES, None), check_vma=False)
```

```python
import functools

import jax
import jax.numpy as jnp
from jax import lax
from jax.experimental import pallas as pl
from jax.experimental.pallas import tpu as pltpu
from jax.sharding import PartitionSpec as P

EPS = 1e-6
GROUP_AXES = ('pool', 'ep')
BATCH_AXES = ('dp', 'pool', 'ep')
MESH = pl.DeviceIdType.MESH
F32 = jnp.float32
BF16 = jnp.bfloat16
VMEM_LIMIT = 66_000_000

NZ, NY = 4, 2
GROUP = 16
TOK = 128
HALF = TOK // 2
D = 896
HEADS, KV, HD, SEQ = 16, 4, 128, 32
PER_KV = HEADS // KV
TOP = 8
EXPERTS, LOCAL, FF = 256, 16, 256
SLOTS = LOCAL * TOK
BLK = 16


def rms(wide):
    return wide * lax.rsqrt(jnp.mean(wide * wide, axis=-1, keepdims=True) + EPS)


def dot(a, b):
    return jnp.dot(a, b, preferred_element_type=F32)


def split3(wide):
    high = wide.astype(BF16)
    rest = wide - high.astype(F32)
    mid = rest.astype(BF16)
    low = (rest - mid.astype(F32)).astype(BF16)
    return high, mid, low


OTHERS = [(dz, dy, dc) for dz in range(NZ) for dy in range(NY) for dc in range(2) if (dz, dy, dc) != (0, 0, 0)]


def position():
    z = lax.axis_index('pool')
    ep = lax.axis_index('ep')
    y = ep // 2
    core = lax.rem(ep, 2)

    def at(zz, dy, dc):
        return {'pool': zz, 'ep': lax.rem(y + dy, 2) * 2 + lax.rem(core + dc, 2)}
    return z, y, core, at


def slot(zz, dy, dc):
    return (zz * 2 + dy) * 2 + dc


def remote(src, dst, send, recv, target):
    return pltpu.make_async_remote_copy(src_ref=src, dst_ref=dst, send_sem=send, recv_sem=recv, device_id=target, device_id_type=MESH)


EDGE = 16
PARTS = ((0, 64), (64, 64))
GATHER = PARTS
HALVES = ((0, EDGE), (EDGE, 48), PARTS[1])
EVEN = ((0, EDGE), (EDGE, 56), (72, 56))
WHOLE = (0, TOK)


def kernel(layers, x_ref, kc_hbm, vc_hbm, len_ref, wq_hbm, wk_hbm, wv_hbm, wo_hbm, wr_hbm, ids_own, wg_hbm, wu_hbm, wd_hbm, out_ref,
           wg, wu, wd, wr, rows, xs, ys, pick, mix, gates, pos, jpos, tgt, base_ref, ids_ref,
           x_s, a_ref, u_ref, gate_ref, qs, ks, vs, mixed,
           core_in, y_in, y_edge, right_in, right_edge, left_in, left_edge,
           wsem, asem, ksem, vsem, isem_s, isem_r, gsem_s, gsem_r, az_s, az_r, ay_s, ay_r, ac_s, ac_r,
           rc_s, rc_r, ry_s, ry_r, rr_s, rr_r, rl_s, rl_r):
    z, y, core, at = position()
    first = (z * 4 + y * 2 + core) * LOCAL
    side = z // 2
    near = z - side * (2 * z - 3)
    mirror = lambda v: v + side * (3 - 2 * v)
    n1, n2, n3 = mirror(1 - near), mirror(2), mirror(3)
    order = (mirror(3), mirror(2), mirror(1 - near), mirror(near))
    inside, end = near == 1, near == 0

    mine = slot(z, 0, 0)
    partner, across = at(z, 0, 1), at(z, 1, 0)
    along = lambda zz: at(zz, 0, 0)
    barrier = pltpu.get_barrier_semaphore()
    for dz, dy, dc in OTHERS:
        pl.semaphore_signal(barrier, inc=1, device_id=at(lax.rem(z + dz, NZ), dy, dc), device_id_type=MESH)

    def attention_loads(layer):
        pairs = [(wq_hbm.at[layer, :, pl.ds(c * FF, FF)], wg.at[c]) for c in range(8)]
        pairs += [(wk_hbm.at[layer, :, pl.ds(c * FF, FF)], wg.at[8 + c]) for c in range(2)]
        pairs += [(wv_hbm.at[layer, :, pl.ds(c * FF, FF)], wg.at[10 + c]) for c in range(2)]
        pairs += [(wo_hbm.at[layer, pl.ds(c * FF, FF)], wd.at[c]) for c in range(8)]
        pairs += [(wr_hbm.at[layer], wr)]
        return [pltpu.make_async_copy(src, dst, asem.at[i]) for i, (src, dst) in enumerate(pairs)]

    def cache_loads(layer):
        copies = []
        for hbm, start, sem in ((kc_hbm, 0, ksem), (vc_hbm, TOK // BLK, vsem)):
            for q in range(BLK):
                copies.append(pltpu.make_async_copy(hbm.at[layer, :, q], pick.at[pl.ds(start, TOK // BLK), :, pl.ds(q * HD, HD)], sem.at[q]))
        return copies

    chunk = 4

    def expert_loads(layer):
        copies = []
        for i in range(LOCAL // chunk):
            part = pl.ds(i * chunk, chunk)
            for j, (src, dst) in enumerate(((wg_hbm, wg), (wu_hbm, wu), (wd_hbm, wd))):
                copies.append(pltpu.make_async_copy(src.at[layer, part], dst.at[part], wsem.at[j, i]))
        return copies

    def start(copies):
        for copy in copies:
            copy.start()

    def ids_copy(dz, dy, dc):
        me = slot(z, dy, dc)
        return remote(ids_own, ids_ref.at[me], isem_s.at[dz * 4 + dy * 2 + dc], isem_r.at[me], at(lax.rem(z + dz, NZ), dy, dc))

    def ids_start():
        pl.semaphore_wait(barrier, len(OTHERS))
        for o in OTHERS:
            ids_copy(*o).start()
        ids_ref[mine] = ids_own[...]

    def ids_wait():
        for dz, dy, dc in OTHERS:
            ids_copy(dz, dy, dc).wait_send()
            i = slot(lax.rem(z + dz, NZ), dy, dc)
            remote(ids_own, ids_ref.at[i], isem_s.at[0], isem_r.at[i], partner).wait_recv()

    scale = HD ** -0.5
    pair_lane = lax.broadcasted_iota(jnp.int32, (HEADS, SEQ * KV), 1)
    pair_head = lax.broadcasted_iota(jnp.int32, (HEADS, SEQ * KV), 0)
    pair_pos = jnp.where(lax.rem(pair_lane, KV) == pair_head // PER_KV, pair_lane // KV, SEQ)

    def attend(b, carry):
        tok = b * BLK
        part = pl.ds(tok * HEADS, BLK * HEADS)
        q_wide = qs[part, :]
        q_blk = q_wide.astype(BF16)
        score_list, mask_list = [], []
        for t in range(BLK):
            keys = pick[b, :, t * HD:(t + 1) * HD]
            score_list.append(lax.dot_general(q_blk[t * HEADS:(t + 1) * HEADS], keys, (((1,), (1,)), ((), ())), preferred_element_type=F32))
            mask_list.append(pair_pos < len_ref[0, tok + t])
        score = jnp.concatenate(score_list, axis=0) * scale
        mask = jnp.concatenate(mask_list, axis=0)
        score = jnp.where(mask, score, -jnp.inf)
        score_new = jnp.sum(q_wide * ks[part, :], axis=-1, keepdims=True) * scale
        peak = jnp.maximum(jnp.max(score, axis=-1, keepdims=True), score_new)
        prob = jnp.exp(score - peak)
        prob_new = jnp.exp(score_new - peak)
        total = jnp.sum(prob, axis=-1, keepdims=True) + prob_new
        prob = (prob / total).astype(BF16)
        prob_new = (prob_new / total).astype(BF16).astype(F32)
        out = [dot(prob[t * HEADS:(t + 1) * HEADS], pick[TOK // BLK + b, :, t * HD:(t + 1) * HD]) for t in range(BLK)]
        out = jnp.concatenate(out, axis=0) + prob_new * vs[part, :]
        qs[part, :] = out.astype(BF16).astype(F32)
        return carry

    def project(layer, span, x_from):
        loads = attention_loads(layer)
        begin, count = span
        with jax.named_scope('qkv'):
            h = rms(x_from[begin:begin + count].astype(F32)).astype(BF16)

            def spread(ref, head, block):
                ref[pl.ds(begin * HEADS + head, count, stride=HEADS), :] = block

            for c in range(8):
                if begin == 0:
                    loads[c].wait()
                q = dot(h, wg[c]).astype(BF16).astype(F32)
                for j in range(2):
                    spread(qs, c * 2 + j, q[:, j * HD:(j + 1) * HD])
            for c in range(2):
                if begin == 0:
                    loads[8 + c].wait()
                    loads[10 + c].wait()
                k_new = dot(h, wg[8 + c]).astype(BF16).astype(F32)
                v_new = dot(h, wg[10 + c]).astype(BF16).astype(F32)
                for i in range(8):
                    j = i // PER_KV
                    spread(ks, c * 8 + i, k_new[:, j * HD:(j + 1) * HD])
                    spread(vs, c * 8 + i, v_new[:, j * HD:(j + 1) * HD])

    def attend_blocks(first_block, stop):
        with jax.named_scope('att'):
            lax.fori_loop(first_block, stop, attend, 0, unroll=2)

    def project_out(layer, span, x_from):
        begin, count = span
        with jax.named_scope('post'):
            for i in range(HEADS):
                mixed[:count, i * HD:(i + 1) * HD] = qs[pl.ds(begin * HEADS + i, count, stride=HEADS), :].astype(BF16)
            if begin == 0:
                for copy in attention_loads(layer)[12:]:
                    copy.wait()
            x = x_from[begin:begin + count].astype(F32)
            a = (x + dot(mixed[:count, :], wd[0:8].reshape(HEADS * HD, D))).astype(BF16)
            a_ref[begin:begin + count] = a
            u_ref[begin:begin + count] = rms(a.astype(F32)).astype(BF16)

    def route(layer):
        with jax.named_scope('route'):
            u = u_ref[...]
            high, mid, low3 = split3(wr[...])
            logits = ((dot(u, low3) + dot(u, mid)) + dot(u, high)).T
            row = lax.broadcasted_iota(jnp.int32, (EXPERTS, TOK), 0)
            chosen = [jnp.sum(jnp.where(row == ids_own[layer, k:k + 1, :], logits, 0.0), axis=0, keepdims=True) for k in range(TOP)]
            chosen = jnp.concatenate(chosen, axis=0)
            weight = jnp.exp(chosen - jnp.max(chosen, axis=0, keepdims=True))
            gate_ref[...] = weight / jnp.sum(weight, axis=0, keepdims=True)

    def send_part(part):
        both_ways(lambda step: own_z_send(part, step), 'start')
        own_y_send(part).start()

    def first_part(layer, span, x_from, between):
        project(layer, span, x_from)
        between(0)
        for copy in cache_loads(layer):
            copy.wait()
        if layer == 0:
            attend_blocks(0, 2)
            with jax.named_scope('barrier'):
                ids_start()
            attend_blocks(2, span[1] // BLK)
        else:
            attend_blocks(0, span[1] // BLK)
        between(1)
        project_out(layer, span, x_from)

    expert = lax.broadcasted_iota(jnp.int32, (LOCAL, TOK), 0) + first
    tri = (lax.broadcasted_iota(jnp.int32, (TOK, TOK), 0) < lax.broadcasted_iota(jnp.int32, (TOK, TOK), 1)).astype(BF16)
    ones = jnp.ones((TOK, TOK), BF16)
    low = (lax.broadcasted_iota(jnp.int32, (LOCAL, LOCAL), 1) < lax.broadcasted_iota(jnp.int32, (LOCAL, LOCAL), 0)).astype(BF16)
    lane = lax.broadcasted_iota(jnp.int32, (LOCAL, TOK), 1).astype(F32)
    sub = lax.broadcasted_iota(jnp.int32, (TOK, TOK), 0).astype(F32)
    sub16 = sub.astype(BF16)

    def onehot(row):
        row16 = jnp.broadcast_to(row, (16, TOK)).astype(BF16)
        return jnp.where(sub16 == jnp.concatenate([row16] * (TOK // 16), axis=0), jnp.ones((TOK, TOK), BF16), jnp.zeros((TOK, TOK), BF16))

    def plan(layer, s, base):
        ids = ids_ref[s, layer]
        hit = jnp.zeros((LOCAL, TOK), F32)
        for k in range(TOP):
            hit = hit + jnp.where(expert == ids[k:k + 1, :], 1.0, 0.0)
        hit16 = hit.astype(BF16)
        rank = dot(hit16, tri)
        count = dot(hit16, ones)
        offset = dot(low, count.astype(BF16))
        pos[s] = jnp.where(hit > 0, base + rank, -1.0)
        jpos[s] = jnp.where(hit > 0, offset + rank, -1.0)
        local = lane - base
        tgt[s] = jnp.where((local >= 0) & (local < count), local + offset, -1.0)
        return base + count

    def plan_part(layer, begin, stop):
        if begin == 0:
            base_ref[...] = jnp.zeros((LOCAL, TOK), F32)
        base_ref[...] = lax.fori_loop(begin, stop, functools.partial(plan, layer), base_ref[...], unroll=2)

    def block(zz, dy, dc, start, count):
        return rows.at[zz * 2 + dy, pl.ds(dc * TOK + start, count)]

    def z_send(zz, c, step):
        if c == 2:
            src = block(zz, 1, 0, 0, EDGE)
        else:
            src = block(zz, 0, 0, *GATHER[c])
        return remote(src, src, az_s.at[zz, c, (step + 1) // 2], az_r.at[zz, c], along(z + step))

    def own_z_send(c, step):
        return remote(u_ref.at[pl.ds(*GATHER[c])], block(z, 0, 0, *GATHER[c]), az_s.at[z, c, (step + 1) // 2], az_r.at[z, c], along(z + step))

    def z_arrival(zz, c):
        src = block(zz, 1, 0, 0, EDGE) if c == 2 else block(zz, 0, 0, *GATHER[c])
        return remote(src, src, az_s.at[zz, c, 0], az_r.at[zz, c], partner)

    def y_piece(c):
        start, count = GATHER[c]
        return (EDGE, count - EDGE) if c == 0 else (start, count)

    def y_send(zz, c):
        return remote(block(zz, 0, 0, *y_piece(c)), block(zz, 1, 0, *y_piece(c)), ay_s.at[zz, c], ay_r.at[zz, c], across)

    def own_y_send(c):
        return remote(u_ref.at[pl.ds(*GATHER[c])], block(z, 1, 0, *GATHER[c]), ay_s.at[z, c], ay_r.at[z, c], across)

    def core_send(zz, dy):
        return remote(block(zz, dy, 0, 0, TOK), block(zz, dy, 1, 0, TOK), ac_s.at[zz, dy], ac_r.at[zz, dy], partner)

    def own_core_send():
        return remote(u_ref, block(z, 0, 1, 0, TOK), ac_s.at[z, 0], ac_r.at[z, 0], partner)

    def both_ways(make, act):
        @pl.when(z < NZ - 1)
        def _():
            getattr(make(1), act)()

        @pl.when(z > 0)
        def _():
            getattr(make(-1), act)()

    def onward(zz, c, act):
        @pl.when((zz < z) & (z < NZ - 1))
        def _():
            getattr(z_send(zz, c, 1), act)()

        @pl.when((zz > z) & (z > 0))
        def _():
            getattr(z_send(zz, c, -1), act)()

    def gate_copy(dz, dy, dc):
        me = slot(z, dy, dc)
        return remote(gate_ref, gates.at[me], gsem_s.at[dz * 4 + dy * 2 + dc], gsem_r.at[me], at(lax.rem(z + dz, NZ), dy, dc))

    per = 4

    def fill(zz, dy, fresh=False):
        chip = zz * 2 + dy

        def body(i, carry):
            picks = []
            for j in range(per):
                e = i * per + j
                picks.append(jnp.concatenate([onehot(pos[chip * 2 + dc, pl.ds(e, 1), :]) for dc in range(2)], axis=1))
            got = dot(jnp.concatenate(picks, axis=0), rows[chip])
            where = pl.ds(pl.multiple_of(i * per * TOK, per * TOK), per * TOK)
            if fresh:
                xs[where, :] = got
            else:
                xs[where, :] += got
            return carry
        with jax.named_scope('fill'):
            core_send(zz, dy).wait_recv()
            lax.fori_loop(0, LOCAL // per, body, 0)

    def arrive(zz, c):
        z_arrival(zz, c).wait_recv()
        onward(zz, c, 'start')
        if c < 2:
            y_send(zz, c).start()
        if c == 1:
            core_send(zz, 0).start()

    def arrive_y(zz):
        for c in range(2):
            y_send(zz, c).wait_recv()
        core_send(zz, 1).start()

    def pick_rows(s, carry):
        for e in range(LOCAL):
            pick[s, :, e * TOK:(e + 1) * TOK] = onehot(tgt[s, e:e + 1, :])
        return carry

    def gather(layer, x_from):
        cut_in_two = layer > 0

        def begin_first():
            arrive(n1, 0)
            pl.when(inside)(lambda: arrive(n2, 0))
            own_y_send(0).wait_recv()
            both_ways(lambda step: z_send(z, 2, step), 'start')

        def edge_first():
            arrive(n1, 2)
            pl.when(inside)(lambda: arrive(n2, 2))

        if cut_in_two:
            middle = (PARTS[1][0] + PARTS[1][1] // 2 + BLK - 1) // BLK
            project(layer, PARTS[1], x_from)
            attend_blocks(PARTS[1][0] // BLK, middle)
            begin_first()
            attend_blocks(middle, TOK // BLK)
            project_out(layer, PARTS[1], x_from)
            send_part(1)
        own_core_send().start()
        start(expert_loads(layer))
        if cut_in_two:
            pl.when(end)(lambda: arrive(n2, 0))
            pl.when(inside)(lambda: arrive(n3, 0))
        route(layer)
        for o in OTHERS:
            gate_copy(*o).start()
        gates[mine] = gate_ref[...]
        rows[z * 2, pl.ds(0, TOK), :] = u_ref[...]
        if layer == 0:
            with jax.named_scope('plan'):
                ids_wait()
                plan_part(0, 0, GROUP)
        if cut_in_two:
            edge_first()
        if not cut_in_two:
            begin_first()
        fill(z, 0, True)
        arrive(n1, 1)
        pl.when(inside)(lambda: arrive(n2, 1))
        own_y_send(1).wait_recv()
        core_send(z, 1).start()
        if cut_in_two:
            pl.when(end)(lambda: arrive(n3, 0))
            pl.when(end)(lambda: arrive(n2, 2))
        with jax.named_scope('picks'):
            lax.fori_loop(0, GROUP // 2, pick_rows, 0)
        fill(n1, 0)
        if not cut_in_two:
            pl.when(end)(lambda: arrive(n2, 0))
            pl.when(inside)(lambda: arrive(n3, 0))
            edge_first()
        pl.when(end)(lambda: arrive(n2, 1))
        pl.when(inside)(lambda: arrive(n3, 1))
        fill(z, 1)
        with jax.named_scope('picks'):
            lax.fori_loop(GROUP // 2, GROUP, pick_rows, 0)
        fill(n2, 0)
        if not cut_in_two:
            pl.when(end)(lambda: arrive(n2, 2))
            pl.when(end)(lambda: arrive(n3, 0))
        arrive_y(n1)
        fill(n1, 1)
        pl.when(end)(lambda: arrive(n3, 1))
        arrive_y(n2)
        fill(n3, 0)
        arrive(n3, 2)
        fill(n2, 1)
        arrive_y(n3)
        fill(n3, 1)

        own_core_send().wait_send()
        for c in range(2):
            own_y_send(c).wait_send()
            both_ways(lambda step: own_z_send(c, step), 'wait_send')
        both_ways(lambda step: z_send(z, 2, step), 'wait_send')
        for zz in (n1, n2, n3):
            core_send(zz, 0).wait_send()
            for c in range(3):
                onward(zz, c, 'wait_send')
                if c < 2:
                    y_send(zz, c).wait_send()
        for zz in range(NZ):
            core_send(zz, 1).wait_send()
        for dz, dy, dc in OTHERS:
            gate_copy(dz, dy, dc).wait_send()
            s = slot(lax.rem(z + dz, NZ), dy, dc)
            remote(gate_ref, gates.at[s], gsem_s.at[0], gsem_r.at[s], partner).wait_recv()

    def ready(layer, s):
        ids = ids_ref[s, layer]
        gate = gates[s]
        g = jnp.zeros((LOCAL, TOK), F32)
        for k in range(TOP):
            g = g + jnp.where(expert == ids[k:k + 1, :], gate[k:k + 1, :], 0.0)
        jp = jpos[s]
        acc = jnp.zeros((TOK, TOK), F32)
        for e in range(LOCAL):
            acc = acc + jnp.where(sub == jp[e:e + 1, :], g[e:e + 1, :], 0.0)
        for i, part in enumerate(split3(acc.T)):
            mix[s, i * TOK:(i + 1) * TOK, :] = part
    def experts(layer, e, carry):
        ready(layer, e)
        window = pl.ds(pl.multiple_of(e * TOK, TOK), TOK)
        x = xs[window, :].astype(BF16)
        inner = (jax.nn.silu(dot(x, wg[e])) * dot(x, wu[e])).astype(BF16)
        ys[window, :] = dot(inner, wd[e]).astype(BF16)
        return carry
    def all_experts(layer):
        with jax.named_scope('experts'):
            weights = expert_loads(layer)
            for i in range(LOCAL // chunk):
                for copy in weights[3 * i:3 * i + 3]:
                    copy.wait()
                lax.fori_loop(i * chunk, (i + 1) * chunk, functools.partial(experts, layer), 0)

    cut = list(HALVES)

    def own_part(i, start=0, count=TOK):
        return xs.at[pl.ds(pl.multiple_of(i * TOK + start, 8), count)]

    def far_part(i):
        return xs.at[pl.ds(pl.multiple_of((NZ * NY + i) * TOK, TOK), TOK)]

    def core_copy(i):
        return remote(far_part(i), core_in.at[i], rc_s.at[i], rc_r.at[i], partner)

    def y_copy(zd, c):
        part = pl.ds(*cut[c])
        if c == 0:
            dst = y_edge
        else:
            dst = y_in.at[zd, part]
        return remote(own_part(zd * 2 + 1, *cut[c]), dst, ry_s.at[zd, c], ry_r.at[zd, c], across)

    def z_copy(zd, c, step, target=None):
        main, edge, send, recv = (right_in, right_edge, rr_s, rr_r) if step == 1 else (left_in, left_edge, rl_s, rl_r)
        target = along(z + step) if target is None else target
        if c == 3:
            return remote(own_part(zd * 2 + 1, 0, EDGE), edge.at[zd], send.at[zd, c], recv.at[zd, c], target)
        return remote(own_part(zd * 2, *cut[c]), main.at[zd, pl.ds(*cut[c])], send.at[zd, c], recv.at[zd, c], target)

    def take(zd, c, step):
        z_copy(zd, c, step, partner).wait_recv()
        main, edge = (right_in, right_edge) if step == 1 else (left_in, left_edge)
        if c == 3:
            own_part(zd * 2 + 1, 0, EDGE)[...] += edge[zd]
        else:
            own_part(zd * 2, *cut[c])[...] += main[zd, pl.ds(*cut[c])]

    def chain(zd, c):
        @pl.when(zd > z)
        def _():
            @pl.when(z > 0)
            def _():
                take(zd, c, 1)
            z_copy(zd, c, 1).start()

        @pl.when(zd < z)
        def _():
            @pl.when(z < NZ - 1)
            def _():
                take(zd, c, -1)
            z_copy(zd, c, -1).start()

    def last(c):
        @pl.when(z > 0)
        def _():
            take(z, c, 1)

        @pl.when(z < NZ - 1)
        def _():
            take(z, c, -1)

    def edge_out():
        last(3)
        y_copy(z, 0).start()

    def edge_in():
        y_copy(z, 0).wait_recv()
        own_part(z * 2, 0, EDGE)[...] += y_edge[...]

    def cross(zd, c):
        y_copy(zd, c).wait_recv()
        own_part(zd * 2, *cut[c])[...] += y_in[zd, pl.ds(*cut[c])]

    def edges(zd):
        chain(zd, 0)
        chain(zd, 3)

    def piece(zd, c):
        cross(zd, c)
        chain(zd, c)

    targets = [order[i] * 2 + dy for i in range(NZ) for dy in (1, 0)]

    def pick_target(j):
        value = targets[0]
        for i in range(1, len(targets)):
            value = jnp.where(j == i, targets[i], value)
        return value

    def finish(more, j):
        i = pick_target(j)
        core_copy(i).wait_recv()
        own_part(i)[...] += core_in[i]

        @pl.when(lax.rem(i, 2) == 1)
        def _():
            y_copy(i // 2, 1).start()
            if not more:
                y_copy(i // 2, 2).start()

    def combine(more, j, carry):
        i = pick_target(j)
        s = i * 2
        pairs = dot(pick[pl.ds(s, 2)].reshape(2 * TOK, SLOTS), ys[...]).astype(BF16)
        for dc, part in ((1, far_part), (0, own_part)):
            got = dot(mix[s + dc], pairs[dc * TOK:(dc + 1) * TOK])
            part(i)[...] = (got[2 * TOK:] + got[TOK:2 * TOK]) + got[:TOK]
            if dc == 1:
                core_copy(i).start()

        @pl.when(j > 0)
        def _():
            finish(more, j - 1)

        @pl.when(end & (j == 2))
        def _():
            edges(order[0])

        @pl.when(end & (j == 4))
        def _():
            edges(order[1])

        @pl.when(end & (j == 5))
        def _():
            piece(order[0], 1)

        @pl.when(end & (j == 7))
        def _():
            if more:
                piece(order[1], 1)
            else:
                piece(order[0], 2)

        @pl.when(inside & (j == 5))
        def _():
            edges(order[0])

        @pl.when(inside & (j == 7))
        def _():
            edges(order[1])
        return carry

    def reduce(layer):
        more = layer + 1 < layers
        cut[:] = HALVES if more else EVEN

        def ahead(i):
            if layer + 1 < layers:
                plan_part(layer + 1, i * 4, i * 4 + 4)

        with jax.named_scope('combine'):
            lax.fori_loop(0, len(targets), functools.partial(combine, more), 0)
        if layer + 1 < layers:
            start(cache_loads(layer + 1))

        dest = x_s if layer + 1 < layers else out_ref

        def done(span):
            begin, count = span
            dest[begin:begin + count] = (a_ref[begin:begin + count].astype(F32) + own_part(z * 2, begin, count)[...]).astype(BF16)

        with jax.named_scope('chain'):
            finish(more, len(targets) - 1)
            if more:
                y_copy(order[0], 2).start()
            edges(order[2])

            @pl.when(inside)
            def _():
                piece(order[0], 1)
            ahead(0)

            if more:
                @pl.when(inside)
                def _():
                    piece(order[1], 1)
                ahead(1)
                edge_out()
                for i in range(1, NZ):
                    y_copy(order[i], 2).start()
                piece(order[2], 1)
                ahead(2)
                last(0)
                ahead(3)
                cross(z, 1)

                @pl.when(end)
                def _():
                    piece(order[0], 2)
                last(1)
                edge_in()
                done(PARTS[0])

            else:
                @pl.when(inside)
                def _():
                    piece(order[0], 2)
                piece(order[1], 1)
                piece(order[1], 2)
                edge_out()
                piece(order[2], 1)
                piece(order[2], 2)
                last(0)
                cross(z, 1)
                last(1)
                edge_in()
        def between(i):
            @pl.when(end)
            def _():
                piece(order[i + 1], 2)
            if i == 0:
                @pl.when(inside)
                def _():
                    piece(order[0], 2)

        if more:
            first_part(layer + 1, PARTS[0], x_s, between)

            @pl.when(inside)
            def _():
                piece(order[1], 2)
                piece(order[2], 2)
            send_part(0)
        with jax.named_scope('final'):
            cross(z, 2)
            last(2)
            if more:
                done(PARTS[1])
            else:
                done(WHOLE)

        for zz in range(NZ):
            for dy in range(2):
                core_copy(zz * 2 + dy).wait_send()
            for c in (1, 2):
                y_copy(zz, c).wait_send()
            for c in range(4):
                @pl.when(zz > z)
                def _():
                    z_copy(zz, c, 1).wait_send()

                @pl.when(zz < z)
                def _():
                    z_copy(zz, c, -1).wait_send()
        y_copy(z, 0).wait_send()


    start(attention_loads(0))
    start(cache_loads(0))
    first_part(0, WHOLE, x_ref, lambda i: None)
    for part in range(2):
        send_part(part)
    for layer in range(layers):
        gather(layer, x_ref if layer == 0 else x_s)
        all_experts(layer)
        if layer + 1 < layers:
            start(attention_loads(layer + 1))
        reduce(layer)


def solution(mesh):
    def device_step(hidden, k_cache, v_cache, lengths, w_query, w_key, w_value, w_out, w_router, expert_ids, w_gate, w_up, w_down):
        layers = expert_ids.shape[0]
        kc = k_cache.reshape(layers, TOK // BLK, BLK, SEQ * KV, HD)
        vc = v_cache.reshape(layers, TOK // BLK, BLK, SEQ * KV, HD)
        ids = jnp.swapaxes(expert_ids, 1, 2)
        vmem = pl.BlockSpec(memory_space=pltpu.VMEM)
        hbm = pl.BlockSpec(memory_space=pl.ANY)
        sem = pltpu.SemaphoreType.DMA
        buf = pltpu.VMEM
        return pl.pallas_call(
            functools.partial(kernel, layers),
            out_shape=jax.ShapeDtypeStruct((TOK, D), BF16),
            in_specs=[vmem, hbm, hbm, pl.BlockSpec(memory_space=pltpu.SMEM), hbm, hbm, hbm, hbm, hbm, vmem, hbm, hbm, hbm],
            out_specs=vmem,
            scratch_shapes=[
                buf((LOCAL, D, FF), BF16), buf((LOCAL, D, FF), BF16), buf((LOCAL, FF, D), BF16), buf((D, EXPERTS), F32),
                buf((NZ * NY, 2 * TOK, D), BF16), buf((SLOTS, D), F32), buf((SLOTS, D), BF16), buf((GROUP, TOK, SLOTS), BF16), buf((GROUP, 3 * TOK, TOK), BF16),
                buf((GROUP, TOP, TOK), F32), buf((GROUP, LOCAL, TOK), F32), buf((GROUP, LOCAL, TOK), F32), buf((GROUP, LOCAL, TOK), F32),
                buf((LOCAL, TOK), F32), buf((GROUP,) + ids.shape, jnp.int32),
                buf((TOK, D), BF16), buf((TOK, D), BF16), buf((TOK, D), BF16), buf((TOP, TOK), F32),
                buf((TOK * HEADS, HD), F32), buf((TOK * HEADS, HD), F32), buf((TOK * HEADS, HD), F32), buf((TOK, HEADS * HD), BF16),
                buf((NZ * NY, TOK, D), F32), buf((NZ, TOK, D), F32), buf((EDGE, D), F32),
                buf((NZ, TOK, D), F32), buf((NZ, EDGE, D), F32), buf((NZ, TOK, D), F32), buf((NZ, EDGE, D), F32),
                sem((3, 4)), sem((21,)), sem((BLK,)), sem((BLK,)), sem((GROUP,)), sem((GROUP,)), sem((GROUP,)), sem((GROUP,)),
                sem((NZ, 3, 2)), sem((NZ, 3)), *[sem((NZ, 2))] * 4,
                *[sem((NZ * NY,))] * 2, *[sem((NZ, 3))] * 2, *[sem((NZ, 4))] * 4,
            ],
            compiler_params=pltpu.CompilerParams(vmem_limit_bytes=67_043_328, collective_id=0, has_side_effects=True),
            name='layers',
        )(hidden, kc, vc, lengths[None], w_query, w_key, w_value, w_out, w_router, ids, w_gate, w_up, w_down)

    cache_spec = P(None, BATCH_AXES, None, None, None)
    expert_spec = P(None, GROUP_AXES, None, None)
    in_specs = (P(BATCH_AXES, None), cache_spec, cache_spec, P(BATCH_AXES), P(), P(), P(), P(), P(), P(None, BATCH_AXES, None), expert_spec, expert_spec, expert_spec)
    return jax.shard_map(device_step, mesh=mesh, in_specs=in_specs, out_specs=P(BATCH_AXES, None), check_vma=False)
```

```python
import functools

import jax
import jax.numpy as jnp
from jax import lax
from jax.experimental import pallas as pl
from jax.experimental.pallas import tpu as pltpu
from jax.sharding import PartitionSpec as P

EPS = 1e-6
GROUP_AXES = ('pool', 'ep')
BATCH_AXES = ('dp', 'pool', 'ep')
MESH = pl.DeviceIdType.MESH
F32 = jnp.float32
BF16 = jnp.bfloat16
VMEM_LIMIT = 66_000_000

NZ, NY = 4, 2
GROUP = 16
TOK = 128
HALF = TOK // 2
D = 896
HEADS, KV, HD, SEQ = 16, 4, 128, 32
PER_KV = HEADS // KV
TOP = 8
EXPERTS, LOCAL, FF = 256, 16, 256
SLOTS = LOCAL * TOK
BLK = 16


def rms(wide):
    return wide * lax.rsqrt(jnp.mean(wide * wide, axis=-1, keepdims=True) + EPS)


def dot(a, b):
    return jnp.dot(a, b, preferred_element_type=F32)


def split3(wide):
    high = wide.astype(BF16)
    rest = wide - high.astype(F32)
    mid = rest.astype(BF16)
    low = (rest - mid.astype(F32)).astype(BF16)
    return high, mid, low


OTHERS = [(dz, dy, dc) for dz in range(NZ) for dy in range(NY) for dc in range(2) if (dz, dy, dc) != (0, 0, 0)]


def position():
    z = lax.axis_index('pool')
    ep = lax.axis_index('ep')
    y = ep // 2
    core = lax.rem(ep, 2)

    def at(zz, dy, dc):
        return {'pool': zz, 'ep': lax.rem(y + dy, 2) * 2 + lax.rem(core + dc, 2)}
    return z, y, core, at


def slot(zz, dy, dc):
    return (zz * 2 + dy) * 2 + dc


def remote(src, dst, send, recv, target):
    return pltpu.make_async_remote_copy(src_ref=src, dst_ref=dst, send_sem=send, recv_sem=recv, device_id=target, device_id_type=MESH)


EDGE = 16
PARTS = ((0, 64), (64, 64))
GATHER = PARTS
HALVES = ((0, EDGE), (EDGE, 48), PARTS[1])
EVEN = ((0, EDGE), (EDGE, 56), (72, 56))
WHOLE = (0, TOK)


def kernel(layers, x_ref, kc_hbm, vc_hbm, len_ref, wq_hbm, wk_hbm, wv_hbm, wo_hbm, wr_hbm, ids_own, wg_hbm, wu_hbm, wd_hbm, out_ref,
           wg, wu, wd, wr, rows, xs, ys, pick, mix, gates, pos, jpos, tgt, base_ref, ids_ref,
           x_s, a_ref, u_ref, gate_ref, qs, ks, vs, mixed,
           core_in, y_in, y_edge, right_in, right_edge, left_in, left_edge,
           wsem, asem, ksem, vsem, isem_s, isem_r, gsem_s, gsem_r, az_s, az_r, ay_s, ay_r, ac_s, ac_r,
           rc_s, rc_r, ry_s, ry_r, rr_s, rr_r, rl_s, rl_r):
    z, y, core, at = position()
    first = (z * 4 + y * 2 + core) * LOCAL
    side = z // 2
    near = z - side * (2 * z - 3)
    mirror = lambda v: v + side * (3 - 2 * v)
    n1, n2, n3 = mirror(1 - near), mirror(2), mirror(3)
    order = (mirror(3), mirror(2), mirror(1 - near), mirror(near))
    inside, end = near == 1, near == 0

    mine = slot(z, 0, 0)
    partner, across = at(z, 0, 1), at(z, 1, 0)
    along = lambda zz: at(zz, 0, 0)
    barrier = pltpu.get_barrier_semaphore()
    for dz, dy, dc in OTHERS:
        pl.semaphore_signal(barrier, inc=1, device_id=at(lax.rem(z + dz, NZ), dy, dc), device_id_type=MESH)

    def attention_loads(layer):
        pairs = [(wq_hbm.at[layer, :, pl.ds(c * FF, FF)], wg.at[c]) for c in range(8)]
        pairs += [(wk_hbm.at[layer, :, pl.ds(c * FF, FF)], wg.at[8 + c]) for c in range(2)]
        pairs += [(wv_hbm.at[layer, :, pl.ds(c * FF, FF)], wg.at[10 + c]) for c in range(2)]
        pairs += [(wo_hbm.at[layer, pl.ds(c * FF, FF)], wd.at[c]) for c in range(8)]
        pairs += [(wr_hbm.at[layer], wr)]
        return [pltpu.make_async_copy(src, dst, asem.at[i]) for i, (src, dst) in enumerate(pairs)]

    def cache_loads(layer):
        copies = []
        for hbm, start, sem in ((kc_hbm, 0, ksem), (vc_hbm, TOK // BLK, vsem)):
            for q in range(BLK):
                copies.append(pltpu.make_async_copy(hbm.at[layer, :, q], pick.at[pl.ds(start, TOK // BLK), :, pl.ds(q * HD, HD)], sem.at[q]))
        return copies

    chunk = 4

    def expert_loads(layer):
        copies = []
        for i in range(LOCAL // chunk):
            part = pl.ds(i * chunk, chunk)
            for j, (src, dst) in enumerate(((wg_hbm, wg), (wu_hbm, wu), (wd_hbm, wd))):
                copies.append(pltpu.make_async_copy(src.at[layer, part], dst.at[part], wsem.at[j, i]))
        return copies

    def start(copies):
        for copy in copies:
            copy.start()

    def ids_copy(dz, dy, dc):
        me = slot(z, dy, dc)
        return remote(ids_own, ids_ref.at[me], isem_s.at[dz * 4 + dy * 2 + dc], isem_r.at[me], at(lax.rem(z + dz, NZ), dy, dc))

    def ids_start():
        pl.semaphore_wait(barrier, len(OTHERS))
        for o in OTHERS:
            ids_copy(*o).start()
        ids_ref[mine] = ids_own[...]

    def ids_wait():
        for dz, dy, dc in OTHERS:
            ids_copy(dz, dy, dc).wait_send()
            i = slot(lax.rem(z + dz, NZ), dy, dc)
            remote(ids_own, ids_ref.at[i], isem_s.at[0], isem_r.at[i], partner).wait_recv()

    scale = HD ** -0.5
    pair_lane = lax.broadcasted_iota(jnp.int32, (HEADS, SEQ * KV), 1)
    pair_head = lax.broadcasted_iota(jnp.int32, (HEADS, SEQ * KV), 0)
    pair_pos = jnp.where(lax.rem(pair_lane, KV) == pair_head // PER_KV, pair_lane // KV, SEQ)

    def attend(b, carry):
        tok = b * BLK
        part = pl.ds(tok * HEADS, BLK * HEADS)
        q_wide = qs[part, :]
        q_blk = q_wide.astype(BF16)
        score_list, mask_list = [], []
        for t in range(BLK):
            keys = pick[b, :, t * HD:(t + 1) * HD]
            score_list.append(lax.dot_general(q_blk[t * HEADS:(t + 1) * HEADS], keys, (((1,), (1,)), ((), ())), preferred_element_type=F32))
            mask_list.append(pair_pos < len_ref[0, tok + t])
        score = jnp.concatenate(score_list, axis=0) * scale
        mask = jnp.concatenate(mask_list, axis=0)
        score = jnp.where(mask, score, -jnp.inf)
        score_new = jnp.sum(q_wide * ks[part, :], axis=-1, keepdims=True) * scale
        peak = jnp.maximum(jnp.max(score, axis=-1, keepdims=True), score_new)
        prob = jnp.exp(score - peak)
        prob_new = jnp.exp(score_new - peak)
        total = jnp.sum(prob, axis=-1, keepdims=True) + prob_new
        prob = (prob / total).astype(BF16)
        prob_new = (prob_new / total).astype(BF16).astype(F32)
        out = [dot(prob[t * HEADS:(t + 1) * HEADS], pick[TOK // BLK + b, :, t * HD:(t + 1) * HD]) for t in range(BLK)]
        out = jnp.concatenate(out, axis=0) + prob_new * vs[part, :]
        qs[part, :] = out.astype(BF16).astype(F32)
        return carry

    def project(layer, span, x_from):
        loads = attention_loads(layer)
        begin, count = span
        with jax.named_scope('qkv'):
            h = rms(x_from[begin:begin + count].astype(F32)).astype(BF16)

            def spread(ref, head, block):
                ref[pl.ds(begin * HEADS + head, count, stride=HEADS), :] = block

            for c in range(8):
                if begin == 0:
                    loads[c].wait()
                q = dot(h, wg[c]).astype(BF16).astype(F32)
                for j in range(2):
                    spread(qs, c * 2 + j, q[:, j * HD:(j + 1) * HD])
            for c in range(2):
                if begin == 0:
                    loads[8 + c].wait()
                    loads[10 + c].wait()
                k_new = dot(h, wg[8 + c]).astype(BF16).astype(F32)
                v_new = dot(h, wg[10 + c]).astype(BF16).astype(F32)
                for i in range(8):
                    j = i // PER_KV
                    spread(ks, c * 8 + i, k_new[:, j * HD:(j + 1) * HD])
                    spread(vs, c * 8 + i, v_new[:, j * HD:(j + 1) * HD])

    def attend_blocks(first_block, stop):
        with jax.named_scope('att'):
            lax.fori_loop(first_block, stop, attend, 0, unroll=2)

    def project_out(layer, span, x_from):
        begin, count = span
        with jax.named_scope('post'):
            for i in range(HEADS):
                mixed[:count, i * HD:(i + 1) * HD] = qs[pl.ds(begin * HEADS + i, count, stride=HEADS), :].astype(BF16)
            if begin == 0:
                for copy in attention_loads(layer)[12:]:
                    copy.wait()
            x = x_from[begin:begin + count].astype(F32)
            a = (x + dot(mixed[:count, :], wd[0:8].reshape(HEADS * HD, D))).astype(BF16)
            a_ref[begin:begin + count] = a
            u_ref[begin:begin + count] = rms(a.astype(F32)).astype(BF16)

    def route(layer):
        with jax.named_scope('route'):
            u = u_ref[...]
            high, mid, low3 = split3(wr[...])
            logits = ((dot(u, low3) + dot(u, mid)) + dot(u, high)).T
            row = lax.broadcasted_iota(jnp.int32, (EXPERTS, TOK), 0)
            chosen = [jnp.sum(jnp.where(row == ids_own[layer, k:k + 1, :], logits, 0.0), axis=0, keepdims=True) for k in range(TOP)]
            chosen = jnp.concatenate(chosen, axis=0)
            weight = jnp.exp(chosen - jnp.max(chosen, axis=0, keepdims=True))
            gate_ref[...] = weight / jnp.sum(weight, axis=0, keepdims=True)

    def send_part(part):
        both_ways(lambda step: own_z_send(part, step), 'start')
        own_y_send(part).start()

    def first_part(layer, span, x_from, between):
        project(layer, span, x_from)
        between(0)
        for copy in cache_loads(layer):
            copy.wait()
        if layer == 0:
            attend_blocks(0, 2)
            with jax.named_scope('barrier'):
                ids_start()
            attend_blocks(2, span[1] // BLK)
        else:
            attend_blocks(0, span[1] // BLK)
        between(1)
        project_out(layer, span, x_from)

    expert = lax.broadcasted_iota(jnp.int32, (LOCAL, TOK), 0) + first
    tri = (lax.broadcasted_iota(jnp.int32, (TOK, TOK), 0) < lax.broadcasted_iota(jnp.int32, (TOK, TOK), 1)).astype(BF16)
    ones = jnp.ones((TOK, TOK), BF16)
    low = (lax.broadcasted_iota(jnp.int32, (LOCAL, LOCAL), 1) < lax.broadcasted_iota(jnp.int32, (LOCAL, LOCAL), 0)).astype(BF16)
    lane = lax.broadcasted_iota(jnp.int32, (LOCAL, TOK), 1).astype(F32)
    sub = lax.broadcasted_iota(jnp.int32, (TOK, TOK), 0).astype(F32)
    sub16 = sub.astype(BF16)

    def onehot(row):
        row16 = jnp.broadcast_to(row, (16, TOK)).astype(BF16)
        return jnp.where(sub16 == jnp.concatenate([row16] * (TOK // 16), axis=0), jnp.ones((TOK, TOK), BF16), jnp.zeros((TOK, TOK), BF16))

    def plan(layer, s, base):
        ids = ids_ref[s, layer]
        hit = jnp.zeros((LOCAL, TOK), F32)
        for k in range(TOP):
            hit = hit + jnp.where(expert == ids[k:k + 1, :], 1.0, 0.0)
        hit16 = hit.astype(BF16)
        rank = dot(hit16, tri)
        count = dot(hit16, ones)
        offset = dot(low, count.astype(BF16))
        pos[s] = jnp.where(hit > 0, base + rank, -1.0)
        jpos[s] = jnp.where(hit > 0, offset + rank, -1.0)
        local = lane - base
        tgt[s] = jnp.where((local >= 0) & (local < count), local + offset, -1.0)
        return base + count

    def plan_part(layer, begin, stop):
        if begin == 0:
            base_ref[...] = jnp.zeros((LOCAL, TOK), F32)
        base_ref[...] = lax.fori_loop(begin, stop, functools.partial(plan, layer), base_ref[...], unroll=2)

    def block(zz, dy, dc, start, count):
        return rows.at[zz * 2 + dy, pl.ds(dc * TOK + start, count)]

    def z_send(zz, c, step):
        if c == 2:
            src = block(zz, 1, 0, 0, EDGE)
        else:
            src = block(zz, 0, 0, *GATHER[c])
        return remote(src, src, az_s.at[zz, c, (step + 1) // 2], az_r.at[zz, c], along(z + step))

    def own_z_send(c, step):
        return remote(u_ref.at[pl.ds(*GATHER[c])], block(z, 0, 0, *GATHER[c]), az_s.at[z, c, (step + 1) // 2], az_r.at[z, c], along(z + step))

    def z_arrival(zz, c):
        src = block(zz, 1, 0, 0, EDGE) if c == 2 else block(zz, 0, 0, *GATHER[c])
        return remote(src, src, az_s.at[zz, c, 0], az_r.at[zz, c], partner)

    def y_piece(c):
        start, count = GATHER[c]
        return (EDGE, count - EDGE) if c == 0 else (start, count)

    def y_send(zz, c):
        return remote(block(zz, 0, 0, *y_piece(c)), block(zz, 1, 0, *y_piece(c)), ay_s.at[zz, c], ay_r.at[zz, c], across)

    def own_y_send(c):
        return remote(u_ref.at[pl.ds(*GATHER[c])], block(z, 1, 0, *GATHER[c]), ay_s.at[z, c], ay_r.at[z, c], across)

    def core_send(zz, dy):
        return remote(block(zz, dy, 0, 0, TOK), block(zz, dy, 1, 0, TOK), ac_s.at[zz, dy], ac_r.at[zz, dy], partner)

    def own_core_send():
        return remote(u_ref, block(z, 0, 1, 0, TOK), ac_s.at[z, 0], ac_r.at[z, 0], partner)

    def both_ways(make, act):
        @pl.when(z < NZ - 1)
        def _():
            getattr(make(1), act)()

        @pl.when(z > 0)
        def _():
            getattr(make(-1), act)()

    def onward(zz, c, act):
        @pl.when((zz < z) & (z < NZ - 1))
        def _():
            getattr(z_send(zz, c, 1), act)()

        @pl.when((zz > z) & (z > 0))
        def _():
            getattr(z_send(zz, c, -1), act)()

    def gate_copy(dz, dy, dc):
        me = slot(z, dy, dc)
        return remote(gate_ref, gates.at[me], gsem_s.at[dz * 4 + dy * 2 + dc], gsem_r.at[me], at(lax.rem(z + dz, NZ), dy, dc))

    per = 4

    def fill(zz, dy, fresh=False):
        chip = zz * 2 + dy

        def body(i, carry):
            picks = []
            for j in range(per):
                e = i * per + j
                picks.append(jnp.concatenate([onehot(pos[chip * 2 + dc, pl.ds(e, 1), :]) for dc in range(2)], axis=1))
            got = dot(jnp.concatenate(picks, axis=0), rows[chip])
            where = pl.ds(pl.multiple_of(i * per * TOK, per * TOK), per * TOK)
            if fresh:
                xs[where, :] = got
            else:
                xs[where, :] += got
            return carry
        with jax.named_scope('fill'):
            core_send(zz, dy).wait_recv()
            lax.fori_loop(0, LOCAL // per, body, 0)

    def arrive(zz, c):
        z_arrival(zz, c).wait_recv()
        onward(zz, c, 'start')
        if c < 2:
            y_send(zz, c).start()
        if c == 1:
            core_send(zz, 0).start()

    def arrive_y(zz):
        for c in range(2):
            y_send(zz, c).wait_recv()
        core_send(zz, 1).start()

    def pick_rows(s, carry):
        for e in range(LOCAL):
            pick[s, :, e * TOK:(e + 1) * TOK] = onehot(tgt[s, e:e + 1, :])
        return carry

    def gather(layer, x_from):
        cut_in_two = layer > 0

        def begin_first():
            arrive(n1, 0)
            pl.when(inside)(lambda: arrive(n2, 0))
            own_y_send(0).wait_recv()
            both_ways(lambda step: z_send(z, 2, step), 'start')

        def edge_first():
            arrive(n1, 2)
            pl.when(inside)(lambda: arrive(n2, 2))

        if cut_in_two:
            middle = (PARTS[1][0] + PARTS[1][1] // 2 + BLK - 1) // BLK
            project(layer, PARTS[1], x_from)
            attend_blocks(PARTS[1][0] // BLK, middle)
            begin_first()
            attend_blocks(middle, TOK // BLK)
            project_out(layer, PARTS[1], x_from)
            send_part(1)
        own_core_send().start()
        start(expert_loads(layer))
        if cut_in_two:
            pl.when(end)(lambda: arrive(n2, 0))
            pl.when(inside)(lambda: arrive(n3, 0))
        route(layer)
        for o in OTHERS:
            gate_copy(*o).start()
        gates[mine] = gate_ref[...]
        rows[z * 2, pl.ds(0, TOK), :] = u_ref[...]
        if layer == 0:
            with jax.named_scope('plan'):
                ids_wait()
                plan_part(0, 0, GROUP)
        if cut_in_two:
            edge_first()
        if not cut_in_two:
            begin_first()
        fill(z, 0, True)
        arrive(n1, 1)
        pl.when(inside)(lambda: arrive(n2, 1))
        own_y_send(1).wait_recv()
        core_send(z, 1).start()
        if cut_in_two:
            pl.when(end)(lambda: arrive(n3, 0))
            pl.when(end)(lambda: arrive(n2, 2))
        with jax.named_scope('picks'):
            lax.fori_loop(0, GROUP // 2, pick_rows, 0)
        fill(n1, 0)
        if not cut_in_two:
            pl.when(end)(lambda: arrive(n2, 0))
            pl.when(inside)(lambda: arrive(n3, 0))
            edge_first()
        pl.when(end)(lambda: arrive(n2, 1))
        pl.when(inside)(lambda: arrive(n3, 1))
        fill(z, 1)
        with jax.named_scope('picks'):
            lax.fori_loop(GROUP // 2, GROUP, pick_rows, 0)
        fill(n2, 0)
        if not cut_in_two:
            pl.when(end)(lambda: arrive(n2, 2))
            pl.when(end)(lambda: arrive(n3, 0))
        arrive_y(n1)
        fill(n1, 1)
        pl.when(end)(lambda: arrive(n3, 1))
        arrive_y(n2)
        fill(n3, 0)
        arrive(n3, 2)
        fill(n2, 1)
        arrive_y(n3)
        fill(n3, 1)

        own_core_send().wait_send()
        for c in range(2):
            own_y_send(c).wait_send()
            both_ways(lambda step: own_z_send(c, step), 'wait_send')
        both_ways(lambda step: z_send(z, 2, step), 'wait_send')
        for zz in (n1, n2, n3):
            core_send(zz, 0).wait_send()
            for c in range(3):
                onward(zz, c, 'wait_send')
                if c < 2:
                    y_send(zz, c).wait_send()
        for zz in range(NZ):
            core_send(zz, 1).wait_send()
        for dz, dy, dc in OTHERS:
            gate_copy(dz, dy, dc).wait_send()
            s = slot(lax.rem(z + dz, NZ), dy, dc)
            remote(gate_ref, gates.at[s], gsem_s.at[0], gsem_r.at[s], partner).wait_recv()

    def ready(layer, s):
        ids = ids_ref[s, layer]
        gate = gates[s]
        g = jnp.zeros((LOCAL, TOK), F32)
        for k in range(TOP):
            g = g + jnp.where(expert == ids[k:k + 1, :], gate[k:k + 1, :], 0.0)
        jp = jpos[s]
        acc = jnp.zeros((TOK, TOK), F32)
        for e in range(LOCAL):
            acc = acc + jnp.where(sub == jp[e:e + 1, :], g[e:e + 1, :], 0.0)
        for i, part in enumerate(split3(acc.T)):
            mix[s, i * TOK:(i + 1) * TOK, :] = part
    def experts(layer, e, carry):
        ready(layer, e)
        window = pl.ds(pl.multiple_of(e * TOK, TOK), TOK)
        x = xs[window, :].astype(BF16)
        inner = (jax.nn.silu(dot(x, wg[e])) * dot(x, wu[e])).astype(BF16)
        ys[window, :] = dot(inner, wd[e]).astype(BF16)
        return carry
    def all_experts(layer):
        with jax.named_scope('experts'):
            weights = expert_loads(layer)
            for i in range(LOCAL // chunk):
                for copy in weights[3 * i:3 * i + 3]:
                    copy.wait()
                lax.fori_loop(i * chunk, (i + 1) * chunk, functools.partial(experts, layer), 0, unroll=2)

    cut = list(HALVES)

    def own_part(i, start=0, count=TOK):
        return xs.at[pl.ds(pl.multiple_of(i * TOK + start, 8), count)]

    def far_part(i):
        return xs.at[pl.ds(pl.multiple_of((NZ * NY + i) * TOK, TOK), TOK)]

    def core_copy(i):
        return remote(far_part(i), core_in.at[i], rc_s.at[i], rc_r.at[i], partner)

    def y_copy(zd, c):
        part = pl.ds(*cut[c])
        if c == 0:
            dst = y_edge
        else:
            dst = y_in.at[zd, part]
        return remote(own_part(zd * 2 + 1, *cut[c]), dst, ry_s.at[zd, c], ry_r.at[zd, c], across)

    def z_copy(zd, c, step, target=None):
        main, edge, send, recv = (right_in, right_edge, rr_s, rr_r) if step == 1 else (left_in, left_edge, rl_s, rl_r)
        target = along(z + step) if target is None else target
        if c == 3:
            return remote(own_part(zd * 2 + 1, 0, EDGE), edge.at[zd], send.at[zd, c], recv.at[zd, c], target)
        return remote(own_part(zd * 2, *cut[c]), main.at[zd, pl.ds(*cut[c])], send.at[zd, c], recv.at[zd, c], target)

    def take(zd, c, step):
        z_copy(zd, c, step, partner).wait_recv()
        main, edge = (right_in, right_edge) if step == 1 else (left_in, left_edge)
        if c == 3:
            own_part(zd * 2 + 1, 0, EDGE)[...] += edge[zd]
        else:
            own_part(zd * 2, *cut[c])[...] += main[zd, pl.ds(*cut[c])]

    def chain(zd, c):
        @pl.when(zd > z)
        def _():
            @pl.when(z > 0)
            def _():
                take(zd, c, 1)
            z_copy(zd, c, 1).start()

        @pl.when(zd < z)
        def _():
            @pl.when(z < NZ - 1)
            def _():
                take(zd, c, -1)
            z_copy(zd, c, -1).start()

    def last(c):
        @pl.when(z > 0)
        def _():
            take(z, c, 1)

        @pl.when(z < NZ - 1)
        def _():
            take(z, c, -1)

    def edge_out():
        last(3)
        y_copy(z, 0).start()

    def edge_in():
        y_copy(z, 0).wait_recv()
        own_part(z * 2, 0, EDGE)[...] += y_edge[...]

    def cross(zd, c):
        y_copy(zd, c).wait_recv()
        own_part(zd * 2, *cut[c])[...] += y_in[zd, pl.ds(*cut[c])]

    def edges(zd):
        chain(zd, 0)
        chain(zd, 3)

    def piece(zd, c):
        cross(zd, c)
        chain(zd, c)

    targets = [order[i] * 2 + dy for i in range(NZ) for dy in (1, 0)]

    def pick_target(j):
        value = targets[0]
        for i in range(1, len(targets)):
            value = jnp.where(j == i, targets[i], value)
        return value

    def finish(more, j):
        i = pick_target(j)
        core_copy(i).wait_recv()
        own_part(i)[...] += core_in[i]

        @pl.when(lax.rem(i, 2) == 1)
        def _():
            y_copy(i // 2, 1).start()
            if not more:
                y_copy(i // 2, 2).start()

    def combine(more, j, carry):
        i = pick_target(j)
        s = i * 2
        pairs = dot(pick[pl.ds(s, 2)].reshape(2 * TOK, SLOTS), ys[...]).astype(BF16)
        for dc, part in ((1, far_part), (0, own_part)):
            got = dot(mix[s + dc], pairs[dc * TOK:(dc + 1) * TOK])
            part(i)[...] = (got[2 * TOK:] + got[TOK:2 * TOK]) + got[:TOK]
            if dc == 1:
                core_copy(i).start()

        @pl.when(j > 0)
        def _():
            finish(more, j - 1)

        @pl.when(end & (j == 2))
        def _():
            edges(order[0])

        @pl.when(end & (j == 4))
        def _():
            edges(order[1])

        @pl.when(end & (j == 5))
        def _():
            piece(order[0], 1)

        @pl.when(end & (j == 7))
        def _():
            if more:
                piece(order[1], 1)
            else:
                piece(order[0], 2)

        @pl.when(inside & (j == 5))
        def _():
            edges(order[0])

        @pl.when(inside & (j == 7))
        def _():
            edges(order[1])
        return carry

    def reduce(layer):
        more = layer + 1 < layers
        cut[:] = HALVES if more else EVEN

        def ahead(i):
            if layer + 1 < layers:
                plan_part(layer + 1, i * 4, i * 4 + 4)

        with jax.named_scope('combine'):
            lax.fori_loop(0, len(targets), functools.partial(combine, more), 0)
        if layer + 1 < layers:
            start(cache_loads(layer + 1))

        dest = x_s if layer + 1 < layers else out_ref

        def done(span):
            begin, count = span
            dest[begin:begin + count] = (a_ref[begin:begin + count].astype(F32) + own_part(z * 2, begin, count)[...]).astype(BF16)

        with jax.named_scope('chain'):
            finish(more, len(targets) - 1)
            if more:
                y_copy(order[0], 2).start()
            edges(order[2])

            @pl.when(inside)
            def _():
                piece(order[0], 1)
            ahead(0)

            if more:
                @pl.when(inside)
                def _():
                    piece(order[1], 1)
                ahead(1)
                edge_out()
                for i in range(1, NZ):
                    y_copy(order[i], 2).start()
                piece(order[2], 1)
                ahead(2)
                last(0)
                ahead(3)
                cross(z, 1)

                @pl.when(end)
                def _():
                    piece(order[0], 2)
                last(1)
                edge_in()
                done(PARTS[0])

            else:
                @pl.when(inside)
                def _():
                    piece(order[0], 2)
                piece(order[1], 1)
                piece(order[1], 2)
                edge_out()
                piece(order[2], 1)
                piece(order[2], 2)
                last(0)
                cross(z, 1)
                last(1)
                edge_in()
        def between(i):
            @pl.when(end)
            def _():
                piece(order[i + 1], 2)
            if i == 0:
                @pl.when(inside)
                def _():
                    piece(order[0], 2)

        if more:
            first_part(layer + 1, PARTS[0], x_s, between)

            @pl.when(inside)
            def _():
                piece(order[1], 2)
                piece(order[2], 2)
            send_part(0)
        with jax.named_scope('final'):
            cross(z, 2)
            last(2)
            if more:
                done(PARTS[1])
            else:
                done(WHOLE)

        for zz in range(NZ):
            for dy in range(2):
                core_copy(zz * 2 + dy).wait_send()
            for c in (1, 2):
                y_copy(zz, c).wait_send()
            for c in range(4):
                @pl.when(zz > z)
                def _():
                    z_copy(zz, c, 1).wait_send()

                @pl.when(zz < z)
                def _():
                    z_copy(zz, c, -1).wait_send()
        y_copy(z, 0).wait_send()


    start(attention_loads(0))
    start(cache_loads(0))
    first_part(0, WHOLE, x_ref, lambda i: None)
    for part in range(2):
        send_part(part)
    for layer in range(layers):
        gather(layer, x_ref if layer == 0 else x_s)
        all_experts(layer)
        if layer + 1 < layers:
            start(attention_loads(layer + 1))
        reduce(layer)


def solution(mesh):
    def device_step(hidden, k_cache, v_cache, lengths, w_query, w_key, w_value, w_out, w_router, expert_ids, w_gate, w_up, w_down):
        layers = expert_ids.shape[0]
        kc = k_cache.reshape(layers, TOK // BLK, BLK, SEQ * KV, HD)
        vc = v_cache.reshape(layers, TOK // BLK, BLK, SEQ * KV, HD)
        ids = jnp.swapaxes(expert_ids, 1, 2)
        vmem = pl.BlockSpec(memory_space=pltpu.VMEM)
        hbm = pl.BlockSpec(memory_space=pl.ANY)
        sem = pltpu.SemaphoreType.DMA
        buf = pltpu.VMEM
        return pl.pallas_call(
            functools.partial(kernel, layers),
            out_shape=jax.ShapeDtypeStruct((TOK, D), BF16),
            in_specs=[vmem, hbm, hbm, pl.BlockSpec(memory_space=pltpu.SMEM), hbm, hbm, hbm, hbm, hbm, vmem, hbm, hbm, hbm],
            out_specs=vmem,
            scratch_shapes=[
                buf((LOCAL, D, FF), BF16), buf((LOCAL, D, FF), BF16), buf((LOCAL, FF, D), BF16), buf((D, EXPERTS), F32),
                buf((NZ * NY, 2 * TOK, D), BF16), buf((SLOTS, D), F32), buf((SLOTS, D), BF16), buf((GROUP, TOK, SLOTS), BF16), buf((GROUP, 3 * TOK, TOK), BF16),
                buf((GROUP, TOP, TOK), F32), buf((GROUP, LOCAL, TOK), F32), buf((GROUP, LOCAL, TOK), F32), buf((GROUP, LOCAL, TOK), F32),
                buf((LOCAL, TOK), F32), buf((GROUP,) + ids.shape, jnp.int32),
                buf((TOK, D), BF16), buf((TOK, D), BF16), buf((TOK, D), BF16), buf((TOP, TOK), F32),
                buf((TOK * HEADS, HD), F32), buf((TOK * HEADS, HD), F32), buf((TOK * HEADS, HD), F32), buf((TOK, HEADS * HD), BF16),
                buf((NZ * NY, TOK, D), F32), buf((NZ, TOK, D), F32), buf((EDGE, D), F32),
                buf((NZ, TOK, D), F32), buf((NZ, EDGE, D), F32), buf((NZ, TOK, D), F32), buf((NZ, EDGE, D), F32),
                sem((3, 4)), sem((21,)), sem((BLK,)), sem((BLK,)), sem((GROUP,)), sem((GROUP,)), sem((GROUP,)), sem((GROUP,)),
                sem((NZ, 3, 2)), sem((NZ, 3)), *[sem((NZ, 2))] * 4,
                *[sem((NZ * NY,))] * 2, *[sem((NZ, 3))] * 2, *[sem((NZ, 4))] * 4,
            ],
            compiler_params=pltpu.CompilerParams(vmem_limit_bytes=67_043_328, collective_id=0, has_side_effects=True),
            name='layers',
        )(hidden, kc, vc, lengths[None], w_query, w_key, w_value, w_out, w_router, ids, w_gate, w_up, w_down)

    cache_spec = P(None, BATCH_AXES, None, None, None)
    expert_spec = P(None, GROUP_AXES, None, None)
    in_specs = (P(BATCH_AXES, None), cache_spec, cache_spec, P(BATCH_AXES), P(), P(), P(), P(), P(), P(None, BATCH_AXES, None), expert_spec, expert_spec, expert_spec)
    return jax.shard_map(device_step, mesh=mesh, in_specs=in_specs, out_specs=P(BATCH_AXES, None), check_vma=False)
```
